1024 devices in a mesh: ta: 32 (over z_lo, x), gz: 4 (over z_hi), xy: 8 (over y, core).
Axes of the slice: x: 4, y: 4, z: 32 (z_hi: 4, z_lo: 8; z = z_hi * 8 + z_lo), core: 2. Of those that a mesh axis runs over, the one named last changes fastest.
Arguments:
- links: float32 [4, 2, 3, 3, 64, 8, 1024], P(None, None, None, None, 'ta', 'gz', 'xy'), may hold values from -1 to 1, as said below
- solutions: float32 [2, 2, 4, 3, 64, 8, 1024], P(None, None, None, None, 'ta', 'gz', 'xy'), may hold values from -6 to 6
Outputs:
- force: float32 [4, 2, 3, 3, 64, 8, 1024], P(None, None, None, None, 'ta', 'gz', 'xy')
The draws below stay inside these ranges and needn't reach their ends.
Inputs may be any that keep to these rules, and one draw needn't show every extreme that they name: Each links[mu] at a site, read as a complex 3 x 3 matrix, is special unitary.
All inputs are finite; a program needn't handle non-finite values.
Results may differ from the reference program's by a relative error of at most 0.0001.
Values sent between devices are 32-bit elements; how exact they have to be, the bound alone decides.
No kernel may reach another device: no remote copies, remote signals or barrier semaphores. Data moves between devices by JAX's collectives and lax.ppermute only.
A program may use at most 32 MiB of HBM per device.

```python
import math
from functools import reduce
import jax
import jax.numpy as jnp
import numpy as np
from jax import lax

Y_LEN = 64
NSOL = 2
NT = 64
NZ = 8
NXY = 1024


def embed_rotation(turning, phase_one, phase_two, first, second):
    zeros = jnp.zeros_like(turning)
    ones = jnp.ones_like(turning)
    real_rows = [[ones if row == column else zeros for column in range(3)] for row in range(3)]
    imaginary_rows = [[zeros for column in range(3)] for row in range(3)]
    cosine = jnp.cos(turning)
    sine = jnp.sin(turning)
    alpha_real = cosine * jnp.cos(phase_one)
    alpha_imaginary = cosine * jnp.sin(phase_one)
    beta_real = sine * jnp.cos(phase_two)
    beta_imaginary = sine * jnp.sin(phase_two)
    real_rows[first][first] = alpha_real
    imaginary_rows[first][first] = alpha_imaginary
    real_rows[first][second] = beta_real
    imaginary_rows[first][second] = beta_imaginary
    real_rows[second][first] = -beta_real
    imaginary_rows[second][first] = beta_imaginary
    real_rows[second][second] = alpha_real
    imaginary_rows[second][second] = -alpha_imaginary
    real_matrix = jnp.stack([jnp.stack(row, 0) for row in real_rows], 0)
    imaginary_matrix = jnp.stack([jnp.stack(row, 0) for row in imaginary_rows], 0)
    return (real_matrix, imaginary_matrix)


def complex_matmul(left, right):
    real_part = jnp.einsum('ab...,bc...->ac...', left[0], right[0]) - jnp.einsum('ab...,bc...->ac...', left[1], right[1])
    imaginary_part = jnp.einsum('ab...,bc...->ac...', left[0], right[1]) + jnp.einsum('ab...,bc...->ac...', left[1], right[0])
    return (real_part, imaginary_part)


def draw_links(key, part):
    subkeys = jax.random.split(key, 9)
    draw_shape = (4, NT, NZ, NXY)
    angles = [jax.random.uniform(subkeys[index], draw_shape, jnp.float32, 0.0, 2.0 * math.pi) for index in range(9)]
    planes = ((0, 1), (1, 2), (0, 2))
    product = None
    for plane_index in range(3):
        rotation = embed_rotation(angles[3 * plane_index], angles[3 * plane_index + 1], angles[3 * plane_index + 2], planes[plane_index][0], planes[plane_index][1])
        product = rotation if product is None else complex_matmul(product, rotation)
    stacked = jnp.stack([product[0], product[1]], 0)
    return jnp.moveaxis(stacked, 3, 0).astype(jnp.float32)


def block_levels(rng, dims, shards, smallest, high):
    def one(position, shards_of):
        draws = jax.random.uniform(jax.random.fold_in(jax.random.fold_in(rng, 6), position), (shards_of,), jnp.float32, smallest / len(shards), high / len(shards))
        return jnp.repeat(jnp.exp(draws), dims[position] // shards_of).reshape((-1,) + (1,) * (len(dims) - position - 1))

    gain = one(*shards[0])
    for cut in shards[1:]:
        gain = gain * one(*cut)
    return gain


def centred(own_key, dims, spread, limit, cuts=(), kind=jnp.bfloat16):
    values = jax.random.normal(own_key, dims, jnp.float32) * spread
    if len(cuts) > 0:
        values = block_levels(own_key, dims, cuts, -0.22, 0.18) * values
    return jnp.clip(values, min=-limit, max=limit).astype(kind)


def setup_inputs(seed: int = 0) -> dict:
    streams_of = jax.random.split(jax.random.key(seed), 3)
    links = draw_links(jax.random.fold_in(streams_of[2], 71), 0)
    solutions = centred(streams_of[1], (NSOL, 2, 4, 3, NT, NZ, NXY), 1.0, 6.0, ((4, 32), (5, 4), (6, 8)), jnp.float32)
    return dict(links=links, solutions=solutions)


HOPPING = 0.125
PLAQUETTE = 0.5


def projectors():
    identity = np.eye(4)
    zeros = np.zeros((4, 4))
    gamma_time = (np.array([[0, 0, 1, 0], [0, 0, 0, 1], [1, 0, 0, 0], [0, 1, 0, 0]]), zeros)
    gamma_depth = (zeros, np.array([[0, 0, 1, 0], [0, 0, 0, -1], [-1, 0, 0, 0], [0, 1, 0, 0]]))
    gamma_across = (zeros, np.array([[0, 0, 0, 1], [0, 0, 1, 0], [0, -1, 0, 0], [-1, 0, 0, 0]]))
    gamma_along = (np.array([[0, 0, 0, -1], [0, 0, 1, 0], [0, 1, 0, 0], [-1, 0, 0, 0]]), zeros)
    result = []
    for gamma_pair in (gamma_time, gamma_depth, gamma_across, gamma_along):
        result.append(((identity - gamma_pair[0], -gamma_pair[1]), (identity + gamma_pair[0], gamma_pair[1])))
    return result


def shift_rows(source, stride, row_length):
    positions = lax.iota(jnp.int32, source.shape[-1]) % row_length
    if stride > 0:
        return jnp.where(positions == row_length - 1, jnp.roll(source, row_length - 1, -1), jnp.roll(source, -1, -1))
    return jnp.where(positions == 0, jnp.roll(source, 1 - row_length, -1), jnp.roll(source, 1, -1))


def displace(source, direction, stride):
    if direction == 0:
        return jnp.roll(source, -stride, axis=-3)
    if direction == 1:
        return jnp.roll(source, -stride, axis=-2)
    if direction == 2:
        return jnp.roll(source, -stride * Y_LEN, axis=-1)
    return shift_rows(source, stride, Y_LEN)


def displace_spinor(source, direction, stride):
    displaced = displace(source, direction, stride)
    if direction == 0:
        positions = lax.iota(jnp.int32, NT)
        boundary = NT - 1 if stride > 0 else 0
        factor = jnp.where(positions == boundary, -1.0, 1.0).astype(source.dtype)
        displaced = displaced * factor[:, None, None]
    return displaced


def matrix_product(left, right):
    left_real, left_imaginary = left[0], left[1]
    right_real, right_imaginary = right[0], right[1]
    real_part = jnp.sum(left_real[:, :, None] * right_real[None] - left_imaginary[:, :, None] * right_imaginary[None], axis=1)
    imaginary_part = jnp.sum(left_real[:, :, None] * right_imaginary[None] + left_imaginary[:, :, None] * right_real[None], axis=1)
    return jnp.stack([real_part, imaginary_part])


def dagger(matrix):
    return jnp.stack([jnp.swapaxes(matrix[0], 0, 1), -jnp.swapaxes(matrix[1], 0, 1)])


def colour_apply(matrix, spinor):
    matrix_real = matrix[0][None, None]
    matrix_imaginary = matrix[1][None, None]
    spinor_real = spinor[:, 0][:, :, None]
    spinor_imaginary = spinor[:, 1][:, :, None]
    real_part = jnp.sum(matrix_real * spinor_real - matrix_imaginary * spinor_imaginary, axis=3)
    imaginary_part = jnp.sum(matrix_real * spinor_imaginary + matrix_imaginary * spinor_real, axis=3)
    return jnp.stack([real_part, imaginary_part], axis=1)


def spin_apply(projector, spinor):
    spinor_real = spinor[:, 0]
    spinor_imaginary = spinor[:, 1]
    rows_real = []
    rows_imaginary = []
    for spin_row in range(4):
        terms_real = []
        terms_imaginary = []
        for spin_column in range(4):
            weight_real = float(projector[0][spin_row, spin_column])
            weight_imaginary = float(projector[1][spin_row, spin_column])
            terms_real.append(weight_real * spinor_real[:, spin_column] - weight_imaginary * spinor_imaginary[:, spin_column])
            terms_imaginary.append(weight_real * spinor_imaginary[:, spin_column] + weight_imaginary * spinor_real[:, spin_column])
        rows_real.append(reduce(jnp.add, terms_real))
        rows_imaginary.append(reduce(jnp.add, terms_imaginary))
    return jnp.stack([jnp.stack(rows_real, 1), jnp.stack(rows_imaginary, 1)], 1)


def spin_outer(upper_spinor, lower_spinor):
    upper_real = upper_spinor[:, 0][:, :, :, None]
    upper_imaginary = upper_spinor[:, 1][:, :, :, None]
    lower_real = lower_spinor[:, 0][:, :, None]
    lower_imaginary = lower_spinor[:, 1][:, :, None]
    real_part = jnp.sum(upper_real * lower_real + upper_imaginary * lower_imaginary, axis=(0, 1))
    imaginary_part = jnp.sum(upper_imaginary * lower_real - upper_real * lower_imaginary, axis=(0, 1))
    return jnp.stack([real_part, imaginary_part])


def traceless_part(matrix):
    real_part = 0.5 * (matrix[0] - jnp.swapaxes(matrix[0], 0, 1))
    imaginary_part = 0.5 * (matrix[1] + jnp.swapaxes(matrix[1], 0, 1))
    trace_third = (imaginary_part[0, 0] + imaginary_part[1, 1] + imaginary_part[2, 2]) / 3.0
    identity = jnp.eye(3, dtype=matrix.dtype).reshape((3, 3) + (1,) * (matrix.ndim - 3))
    imaginary_part = imaginary_part - identity * trace_third
    return jnp.stack([real_part, imaginary_part])


def reference(links, solutions):
    projector_list = projectors()
    hop_terms = []
    for direction in range(4):
        minus_projector, plus_projector = projector_list[direction]
        forward = colour_apply(links[direction], spin_apply(minus_projector, displace_spinor(solutions, direction, 1)))
        backward = colour_apply(dagger(displace(links[direction], direction, -1)), spin_apply(plus_projector, displace_spinor(solutions, direction, -1)))
        hop_terms.append(forward + backward)
    partner = solutions - HOPPING * reduce(jnp.add, hop_terms)
    forces = []
    for direction in range(4):
        minus_projector, plus_projector = projector_list[direction]
        link_main = links[direction]
        pieces = []
        for second in range(4):
            if second == direction:
                continue
            link_second = links[second]
            upper_staple = matrix_product(matrix_product(displace(link_second, direction, 1), dagger(displace(link_main, second, 1))), dagger(link_second))
            shifted_back = displace(link_second, second, -1)
            lower_staple = matrix_product(matrix_product(dagger(displace(shifted_back, direction, 1)), dagger(displace(link_main, second, -1))), shifted_back)
            pieces.append(upper_staple + lower_staple)
        staple = reduce(jnp.add, pieces)
        fermion = spin_outer(spin_apply(minus_projector, displace_spinor(solutions, direction, 1)), partner) + spin_outer(spin_apply(plus_projector, displace_spinor(partner, direction, 1)), solutions)
        forces.append(traceless_part(matrix_product(link_main, PLAQUETTE * staple + HOPPING * fermion)))
    return jnp.stack(forces)
```

```python
import jax
import jax.numpy as jnp
from jax import lax
from jax.experimental import pallas as pl
from jax.experimental.pallas import tpu as pltpu
from jax.sharding import PartitionSpec as P


HOPPING = 0.125
PLAQUETTE = 0.5
INTERPRET = False

BLOCKS = (
    ((0, 1), (1, 1)),
    ((0, 1j), (1, -1j)),
    ((1, 1j), (0, 1j)),
    ((1, -1), (0, 1)),
)
T, Z, R, Y = 0, 1, 2, 3
OFF = ((0, 1), (0, 2), (1, 2))
ROWS = tuple((a, b) for a in range(2) for b in range(3))
SPINS = tuple((n, s, c) for n in range(2) for s in range(2) for c in range(3))


def add_phase(a, phase, b):
    if phase == 1:
        return (a[0] + b[0], a[1] + b[1])
    if phase == -1:
        return (a[0] - b[0], a[1] - b[1])
    if phase == 1j:
        return (a[0] - b[1], a[1] + b[0])
    return (a[0] + b[1], a[1] - b[0])


def cmul(a, b):
    return (a[0] * b[0] - a[1] * b[1], a[0] * b[1] + a[1] * b[0])


def cmulc(a, b):
    return (a[0] * b[0] + a[1] * b[1], a[1] * b[0] - a[0] * b[1])


def conj(a):
    return (a[0], -a[1])


def csum(terms):
    re, im = terms[0]
    for t in terms[1:]:
        re, im = re + t[0], im + t[1]
    return (re, im)


def csub(a, b):
    return (a[0] - b[0], a[1] - b[1])


def matmul(left, right):
    return [[csum([cmul(left[a][k], right[k][b]) for k in range(3)]) for b in range(3)] for a in range(3)]


def matmul_dagger(left, right):
    return [[csum([cmulc(left[a][k], right[b][k]) for k in range(3)]) for b in range(3)] for a in range(3)]


def third_row(m):
    u, v = m
    cross = lambda i, j: conj(csub(cmul(u[i], v[j]), cmul(u[j], v[i])))
    return [u, v, [cross(1, 2), cross(2, 0), cross(0, 1)]]


def antihermitian(m, scale):
    out = []
    for a, b in OFF:
        out.append((0.5 * scale) * (m[a][b][0] - m[b][a][0]))
        out.append((0.5 * scale) * (m[a][b][1] + m[b][a][1]))
    third = (m[0][0][1] + m[1][1][1] + m[2][2][1]) * (1.0 / 3.0)
    out.append(scale * (m[0][0][1] - third))
    out.append(scale * (m[1][1][1] - third))
    return out


def transport(x, w):
    e = {}
    for i, (a, b) in enumerate(OFF):
        e[a, b] = (x[2 * i], x[2 * i + 1])
        e[b, a] = (-x[2 * i], x[2 * i + 1])
    d = (x[6], x[7], -(x[6] + x[7]))
    v = []
    for a in range(3):
        row = []
        for j in range(3):
            terms = [(-d[a] * w[a][j][1], d[a] * w[a][j][0])]
            terms += [cmul(e[a, b], w[b][j]) for b in range(3) if b != a]
            row.append(csum(terms))
        v.append(row)
    out = []
    for i, j in OFF:
        t = csum([cmulc(v[a][j], w[a][i]) for a in range(3)])
        out += [t[0], t[1]]
    for i in range(2):
        s = None
        for a in range(3):
            p = v[a][i][1] * w[a][i][0] - v[a][i][0] * w[a][i][1]
            s = p if s is None else s + p
        out.append(s)
    return out


class Sites:
    def __init__(self):
        rows = lax.broadcasted_iota(jnp.int32, (4, 128), 0)
        lanes = lax.broadcasted_iota(jnp.int32, (4, 128), 1)
        self.first = (rows < 2, rows % 2 == 0, lanes < 64)
        self.y_last = lanes % 64 == 63
        self.y_first = lanes % 64 == 0

    def swap(self, v, d):
        if d == R:
            return pltpu.roll(v, 64, 1)
        if d == T:
            return jnp.concatenate([v[2:4], v[0:2]], axis=0)
        return jnp.where(
            self.first[Z],
            jnp.concatenate([v[1:4], v[0:1]], axis=0),
            jnp.concatenate([v[3:4], v[0:3]], axis=0),
        )

    def pack_low(self, a, b, d):
        return jnp.where(self.first[d], a, self.swap(b, d))

    def pack_high(self, a, b, d):
        return jnp.where(self.first[d], self.swap(b, d), a)

    def ahead(self, a, b, m, d):
        return (
            self.swap(jnp.where(self.first[d], m, a), d),
            jnp.where(self.first[d], self.swap(b, d), m),
        )

    def behind(self, a, b, m, d):
        return (
            self.swap(jnp.where(self.first[d], a, m), d),
            jnp.where(self.first[d], m, self.swap(b, d)),
        )

    def y_ahead(self, v):
        return jnp.where(self.y_last, pltpu.roll(v, 63, 1), pltpu.roll(v, 127, 1))

    def y_behind(self, v):
        return jnp.where(self.y_first, pltpu.roll(v, 65, 1), pltpu.roll(v, 1, 1))


def link(ref, mu, rows=3):
    return [[tuple(ref[(mu * 2 + c) * 9 + a * 3 + b] for c in range(2)) for b in range(3)] for a in range(rows)]


def spinor(ref, n, s, c):
    return tuple(ref[((n * 2 + k) * 4 + s) * 3 + c] for k in range(2))


def upper(ref, mu, sign, n, s, c):
    col, phase = BLOCKS[mu][s]
    return add_phase(spinor(ref, n, s, c), sign * phase, spinor(ref, n, 2 + col, c))


def half(ref, mu, sign):
    return {k: upper(ref, mu, sign, *k) for k in SPINS}


def flat_half(h):
    return [h[k][c] for k in SPINS for c in range(2)]


def unflat_half(flat):
    return {k: (flat[2 * i], flat[2 * i + 1]) for i, k in enumerate(SPINS)}


def apply(m, h):
    return {(n, s, a): csum([cmul(m[a][b], h[n, s, b]) for b in range(3)]) for n, s, a in SPINS}


def apply_dagger(m, h):
    return {(n, s, a): csum([cmulc(h[n, s, b], m[b][a]) for b in range(3)]) for n, s, a in SPINS}


def others(d):
    return [nu for nu in range(4) if nu != d]


def low_values(lref, xref, d):
    out = []
    for nu in others(d):
        m = link(lref, nu, 2)
        out += [m[a][b][c] for a, b in ROWS for c in range(2)]
    return out + flat_half(half(xref, d, -1))


def put(ref, at, flat):
    for i, v in enumerate(flat):
        ref[at + i] = v


def get(ref, at, n):
    return [ref[at + i] for i in range(n)]


def pack_kernel(flags, lref, xref, zd, zu, ta, tb, ra, rb, gref):
    sites = Sites()
    g = []
    for d in range(3):
        flat = flat_half(apply_dagger(link(lref, d), half(xref, d, 1)))
        put(gref, 24 * d, flat)
        g.append(flat)
    for d in (Z, T, R):
        low = low_values(lref, xref, d)
        low_out = [sites.pack_low(low[2 * i], low[2 * i + 1], d) for i in range(30)]
        high_out = [sites.pack_high(g[d][2 * i], g[d][2 * i + 1], d) for i in range(12)]
        if d == T:
            low_out = low_out[:18] + [jnp.where(flags[0] == 0, -v, v) for v in low_out[18:]]
            high_out = [jnp.where(flags[1] == 0, -v, v) for v in high_out]
        if d == Z:
            put(zd, 0, low_out)
            put(zu, 0, high_out)
            continue
        swap_put(flags[2 + d // 2], (ta, tb) if d == T else (ra, rb), low_out, high_out)


def swap_put(even, refs, low, high):
    flag = even == 1
    for i in range(max(len(low), len(high))):
        a = low[i] if i < len(low) else high[i]
        b = high[i] if i < len(high) else low[i]
        refs[0][i] = jnp.where(flag, b, a)
        refs[1][i] = jnp.where(flag, a, b)


def swap_get(even, refs, n, low):
    flag = even == 1
    first, second = refs if low else (refs[1], refs[0])
    return [jnp.where(flag, first[i], second[i]) for i in range(n)]


def local_kernel(lref, xref, yref, wref, gyref, m2ref):
    sites = Sites()
    u = link(lref, Y)
    h = {k: tuple(sites.y_ahead(v) for v in c) for k, c in half(xref, Y, -1).items()}
    w = apply(u, h)
    g = {k: tuple(sites.y_behind(v) for v in c) for k, c in apply_dagger(u, half(xref, Y, 1)).items()}
    put(wref, 0, flat_half(w))
    put(gyref, 0, flat_half(g))
    for n in range(2):
        for s in range(2):
            for c in range(3):
                x = spinor(xref, n, s, c)
                store_spinor(yref, n, s, c, [x[i] - HOPPING * (w[n, s, c][i] + g[n, s, c][i]) for i in range(2)])
        for r in range(2):
            col, phase = BLOCKS[Y][r]
            for c in range(3):
                x = spinor(xref, n, 2 + col, c)
                diff = [g[n, r, c][i] - w[n, r, c][i] for i in range(2)]
                term = add_phase((0.0, 0.0), complex(phase).conjugate(), diff)
                store_spinor(yref, n, 2 + col, c, [x[i] - HOPPING * term[i] for i in range(2)])
    for mu in range(3):
        m = [[tuple(sites.y_ahead(v) for v in e) for e in row] for row in link(lref, mu)]
        m2 = matmul(u, m)
        put(m2ref, 18 * mu, [m2[a][b][c] for a in range(3) for b in range(3) for c in range(2)])


def store_spinor(ref, n, s, c, value):
    for k in range(2):
        ref[((n * 2 + k) * 4 + s) * 3 + c] = value[k]


def mat_at(ref, at):
    return [[(ref[at + (a * 3 + b) * 2], ref[at + (a * 3 + b) * 2 + 1]) for b in range(3)] for a in range(3)]


def put_mat(ref, at, m):
    put(ref, at, [m[a][b][c] for a in range(3) for b in range(3) for c in range(2)])


def middle_kernel(
    flags, lref, xref, gref, ylref, wyref, gyref, m2ref, zd, zu, ta, tb, ra, rb,
    ozu, ozd, ota, otb, ora, orb, oe, on, obase, oy, ow, nyref, fref, gsref,
):
    sites = Sites()
    put(oy, 0, get(ylref, 0, 48))
    put(ow, 72, get(wyref, 0, 24))
    slot = {}
    for d in range(3):
        if d == Z:
            low_in, high_in = get(zd, 0, 30), get(zu, 0, 12)
        else:
            refs = (ta, tb) if d == T else (ra, rb)
            low_in = swap_get(flags[2 + d // 2], refs, 30, True)
            high_in = swap_get(flags[2 + d // 2], refs, 12, False)
        own = low_values(lref, xref, d)
        ahead = []
        for i in range(30):
            ahead += sites.ahead(own[2 * i], own[2 * i + 1], low_in[i], d)
        for k, nu in enumerate(others(d)):
            f = ahead[12 * k : 12 * k + 12]
            two = [[(f[(a * 3 + b) * 2], f[(a * 3 + b) * 2 + 1]) for b in range(3)] for a in range(2)]
            put_mat(fref, 18 * (3 * d + k), third_row(two))
            slot[d, nu] = 18 * (3 * d + k)
        own = get(gref, 24 * d, 24)
        behind = []
        for i in range(12):
            behind += sites.behind(own[2 * i], own[2 * i + 1], high_in[i], d)
        put(gsref, 24 * d, behind)
        g = unflat_half(behind)
        w = apply(link(lref, d), unflat_half(ahead[36:]))
        put(ow, 24 * d, flat_half(w))
        for n in range(2):
            for s in range(2):
                for c in range(3):
                    y = spinor(oy, n, s, c)
                    store_spinor(oy, n, s, c, [y[i] - HOPPING * (w[n, s, c][i] + g[n, s, c][i]) for i in range(2)])
            for r in range(2):
                col, phase = BLOCKS[d][r]
                for c in range(3):
                    y = spinor(oy, n, 2 + col, c)
                    diff = [HOPPING * (g[n, r, c][i] - w[n, r, c][i]) for i in range(2)]
                    y = add_phase(y, -complex(phase).conjugate(), diff)
                    store_spinor(oy, n, 2 + col, c, y)
    base = [[0.0] * 8 for _ in range(4)]
    lower = {}
    for mu in range(4):
        for nu in range(mu + 1, 4):
            u_mu, u_nu = link(lref, mu), link(lref, nu)
            m1 = matmul(u_mu, mat_at(fref, slot[mu, nu]))
            m2 = mat_at(m2ref, 18 * mu) if nu == Y else matmul(u_nu, mat_at(fref, slot[nu, mu]))
            p = antihermitian(matmul_dagger(m1, m2), PLAQUETTE)
            base[mu] = [a + b for a, b in zip(base[mu], p)]
            base[nu] = [a - b for a, b in zip(base[nu], p)]
            lower[mu, nu] = [-v for v in transport(p, u_nu)]
            lower[nu, mu] = transport(p, u_mu)
    for mu in range(3):
        moved = [sites.y_behind(v) for v in lower[mu, Y]]
        base[mu] = [a + b for a, b in zip(base[mu], moved)]
    for mu in range(4):
        put(obase, 8 * mu, base[mu])
    for d in range(4):
        g = unflat_half(get(gsref, 24 * d, 24) if d < 3 else get(gyref, 0, 24))
        k = half(oy, d, 1)
        m = [
            [csum([cmulc(k[n, s, a], g[n, s, b]) for n in range(2) for s in range(2)]) for b in range(3)]
            for a in range(3)
        ]
        part = antihermitian(m, HOPPING)
        if d == Y:
            put(nyref, 0, [sites.y_ahead(v) for v in part])
            continue
        put(on, 8 * d, part)
        low_out = [sites.pack_low(part[2 * i], part[2 * i + 1], d) for i in range(4)]
        up = []
        for mu in others(d):
            up += lower[mu, d]
        put(oe, 24 * d, up)
        high_out = [sites.pack_high(up[2 * i], up[2 * i + 1], d) for i in range(12)]
        if d == Z:
            put(ozd, 0, low_out)
            put(ozu, 0, high_out)
        else:
            swap_put(flags[2 + d // 2], (ota, otb) if d == T else (ora, orb), low_out, high_out)


def inner_kernel(lref, yref, wref, nyref, baseref, oref):
    for mu in range(4):
        w = unflat_half(get(wref, 24 * mu, 24))
        k = half(yref, mu, -1)
        m = [
            [csum([cmulc(w[n, s, a], k[n, s, b]) for n in range(2) for s in range(2)]) for b in range(3)]
            for a in range(3)
        ]
        part = antihermitian(m, HOPPING)
        total = [a + b for a, b in zip(part, get(baseref, 8 * mu, 8))]
        if mu == Y:
            u = link(lref, Y)
            w_dagger = [[conj(u[j][a]) for j in range(3)] for a in range(3)]
            total = [a + b for a, b in zip(total, transport(get(nyref, 0, 8), w_dagger))]
        put(oref, 8 * mu, total)


def last_kernel(flags, lref, baseref, eref, nref, zu, zd, ta, tb, ra, rb, oref):
    sites = Sites()
    total = [get(baseref, 8 * mu, 8) for mu in range(4)]
    for d in range(3):
        if d == Z:
            low_in, high_in = get(zd, 0, 4), get(zu, 0, 12)
        else:
            refs = (ta, tb) if d == T else (ra, rb)
            low_in = swap_get(flags[2 + d // 2], refs, 4, True)
            high_in = swap_get(flags[2 + d // 2], refs, 12, False)
        own = get(eref, 24 * d, 24)
        behind = []
        for i in range(12):
            behind += sites.behind(own[2 * i], own[2 * i + 1], high_in[i], d)
        for k, mu in enumerate(others(d)):
            total[mu] = [a + b for a, b in zip(total[mu], behind[8 * k : 8 * k + 8])]
        own = get(nref, 8 * d, 8)
        ahead = []
        for i in range(4):
            ahead += sites.ahead(own[2 * i], own[2 * i + 1], low_in[i], d)
        u = link(lref, d)
        w_dagger = [[conj(u[j][a]) for j in range(3)] for a in range(3)]
        total[d] = [a + b for a, b in zip(total[d], transport(ahead, w_dagger))]
    zero = jnp.zeros((4, 128), jnp.float32)
    for mu in range(4):
        x = total[mu]
        at = mu * 18
        for i, (a, b) in enumerate(OFF):
            oref[at + a * 3 + b] = x[2 * i]
            oref[at + b * 3 + a] = -x[2 * i]
            oref[at + 9 + a * 3 + b] = x[2 * i + 1]
            oref[at + 9 + b * 3 + a] = x[2 * i + 1]
        for a in range(3):
            oref[at + a * 4] = zero
        oref[at + 9] = x[6]
        oref[at + 13] = x[7]
        oref[at + 17] = -(x[6] + x[7])


def call(body, operands, outs, flops, scratch=()):
    specs = [
        pl.BlockSpec(memory_space=pltpu.SMEM if o.dtype == jnp.int32 else pltpu.VMEM) for o in operands
    ]
    return pl.pallas_call(
        body,
        in_specs=specs,
        out_specs=[pl.BlockSpec(memory_space=pltpu.VMEM) for _ in outs],
        out_shape=[jax.ShapeDtypeStruct((n, 4, 128), jnp.float32) for n in outs],
        scratch_shapes=[pltpu.VMEM((n, 4, 128), jnp.float32) for n in scratch],
        cost_estimate=pl.CostEstimate(flops=flops, bytes_accessed=4 * 512 * 200, transcendentals=0),
        compiler_params=pltpu.CompilerParams(vmem_limit_bytes=8 * 1024 * 1024),
        interpret=INTERPRET,
    )(*operands)


def move(x, axis, by):
    size = lax.axis_size(axis)
    return lax.ppermute(x, axis, [(i, (i + by) % size) for i in range(size)])


def meet(x, axis, first):
    size = lax.axis_size(axis)
    pairs = []
    for i in range(0 if first else 1, size, 2):
        j = (i + 1) % size
        pairs += [(i, j), (j, i)]
    return lax.ppermute(x, axis, pairs)


def exchange(zd, zu, ta, tb, ra, rb):
    moves = {
        "zd": lambda: move(zd, "gz", -1),
        "zu": lambda: move(zu, "gz", 1),
        "ta": lambda: meet(ta, "ta", True),
        "tb": lambda: meet(tb, "ta", False),
        "ra": lambda: meet(ra, "xy", True),
        "rb": lambda: meet(rb, "xy", False),
    }
    out = {}
    for name in moves:
        out[name] = moves[name]()
    return [out[name] for name in moves]


def on_device(links, solutions):
    shape = links.shape
    lk = links.reshape(72, 4, 128)
    xs = solutions.reshape(48, 4, 128)
    t, r = lax.axis_index("ta"), lax.axis_index("xy")
    flags = jnp.stack([t, lax.axis_size("ta") - 1 - t, 1 - t % 2, 1 - r % 2]).astype(jnp.int32)
    zd, zu, ta, tb, ra, rb, g = call(pack_kernel, (flags, lk, xs), (30, 12, 30, 30, 30, 30, 72), 4_000_000)
    zd, zu, ta, tb, ra, rb = exchange(zd, zu, ta, tb, ra, rb)
    yl, wy, gy, m2 = call(local_kernel, (lk, xs), (48, 24, 24, 54), 20_000_000)
    ozu, ozd, ota, otb, ora, orb, e, n, base, y, w, ny = call(
        middle_kernel,
        (flags, lk, xs, g, yl, wy, gy, m2, zd, zu, ta, tb, ra, rb),
        (12, 4, 12, 12, 12, 12, 72, 24, 32, 48, 96, 8),
        20_000_000,
        (162, 72),
    )
    ozd, ozu, ota, otb, ora, orb = exchange(ozd, ozu, ota, otb, ora, orb)
    (base,) = call(inner_kernel, (lk, y, w, ny, base), (32,), 20_000_000)
    (force,) = call(last_kernel, (flags, lk, base, e, n, ozu, ozd, ota, otb, ora, orb), (72,), 4_000_000)
    return force.reshape(shape)


def solution(mesh):
    spec = P(None, None, None, None, "ta", "gz", "xy")

    return jax.shard_map(on_device, mesh=mesh, in_specs=(spec, spec), out_specs=spec, check_vma=False)
```

```python
import jax
import jax.numpy as jnp
from jax import lax
from jax.experimental import pallas as pl
from jax.experimental.pallas import tpu as pltpu
from jax.sharding import PartitionSpec as P


HOPPING = 0.125
PLAQUETTE = 0.5
INTERPRET = False

BLOCKS = (
    ((0, 1), (1, 1)),
    ((0, 1j), (1, -1j)),
    ((1, 1j), (0, 1j)),
    ((1, -1), (0, 1)),
)
T, Z, R, Y = 0, 1, 2, 3
OFF = ((0, 1), (0, 2), (1, 2))
ROWS = tuple((a, b) for a in range(2) for b in range(3))
SPINS = tuple((n, s, c) for n in range(2) for s in range(2) for c in range(3))


def add_phase(a, phase, b):
    if phase == 1:
        return (a[0] + b[0], a[1] + b[1])
    if phase == -1:
        return (a[0] - b[0], a[1] - b[1])
    if phase == 1j:
        return (a[0] - b[1], a[1] + b[0])
    return (a[0] + b[1], a[1] - b[0])


def cmul(a, b):
    return (a[0] * b[0] - a[1] * b[1], a[0] * b[1] + a[1] * b[0])


def cmulc(a, b):
    return (a[0] * b[0] + a[1] * b[1], a[1] * b[0] - a[0] * b[1])


def conj(a):
    return (a[0], -a[1])


def csum(terms):
    re, im = terms[0]
    for t in terms[1:]:
        re, im = re + t[0], im + t[1]
    return (re, im)


def csub(a, b):
    return (a[0] - b[0], a[1] - b[1])


def matmul(left, right):
    return [[csum([cmul(left[a][k], right[k][b]) for k in range(3)]) for b in range(3)] for a in range(3)]


def matmul_dagger(left, right):
    return [[csum([cmulc(left[a][k], right[b][k]) for k in range(3)]) for b in range(3)] for a in range(3)]


def third_row(m):
    u, v = m
    cross = lambda i, j: conj(csub(cmul(u[i], v[j]), cmul(u[j], v[i])))
    return [u, v, [cross(1, 2), cross(2, 0), cross(0, 1)]]


def antihermitian(m, scale):
    out = []
    for a, b in OFF:
        out.append((0.5 * scale) * (m[a][b][0] - m[b][a][0]))
        out.append((0.5 * scale) * (m[a][b][1] + m[b][a][1]))
    third = (m[0][0][1] + m[1][1][1] + m[2][2][1]) * (1.0 / 3.0)
    out.append(scale * (m[0][0][1] - third))
    out.append(scale * (m[1][1][1] - third))
    return out


def transport(x, w):
    e = {}
    for i, (a, b) in enumerate(OFF):
        e[a, b] = (x[2 * i], x[2 * i + 1])
        e[b, a] = (-x[2 * i], x[2 * i + 1])
    d = (x[6], x[7], -(x[6] + x[7]))
    v = []
    for a in range(3):
        row = []
        for j in range(3):
            terms = [(-d[a] * w[a][j][1], d[a] * w[a][j][0])]
            terms += [cmul(e[a, b], w[b][j]) for b in range(3) if b != a]
            row.append(csum(terms))
        v.append(row)
    out = []
    for i, j in OFF:
        t = csum([cmulc(v[a][j], w[a][i]) for a in range(3)])
        out += [t[0], t[1]]
    for i in range(2):
        s = None
        for a in range(3):
            p = v[a][i][1] * w[a][i][0] - v[a][i][0] * w[a][i][1]
            s = p if s is None else s + p
        out.append(s)
    return out


class Sites:
    def __init__(self):
        rows = lax.broadcasted_iota(jnp.int32, (4, 128), 0)
        lanes = lax.broadcasted_iota(jnp.int32, (4, 128), 1)
        self.first = (rows < 2, rows % 2 == 0, lanes < 64)
        self.y_last = lanes % 64 == 63
        self.y_first = lanes % 64 == 0

    def swap(self, v, d):
        if d == R:
            return pltpu.roll(v, 64, 1)
        if d == T:
            return jnp.concatenate([v[2:4], v[0:2]], axis=0)
        return jnp.where(
            self.first[Z],
            jnp.concatenate([v[1:4], v[0:1]], axis=0),
            jnp.concatenate([v[3:4], v[0:3]], axis=0),
        )

    def pack_low(self, a, b, d):
        return jnp.where(self.first[d], a, self.swap(b, d))

    def pack_high(self, a, b, d):
        return jnp.where(self.first[d], self.swap(b, d), a)

    def ahead(self, a, b, m, d):
        return (
            self.swap(jnp.where(self.first[d], m, a), d),
            jnp.where(self.first[d], self.swap(b, d), m),
        )

    def behind(self, a, b, m, d):
        return (
            self.swap(jnp.where(self.first[d], a, m), d),
            jnp.where(self.first[d], m, self.swap(b, d)),
        )

    def y_ahead(self, v):
        return jnp.where(self.y_last, pltpu.roll(v, 63, 1), pltpu.roll(v, 127, 1))

    def y_behind(self, v):
        return jnp.where(self.y_first, pltpu.roll(v, 65, 1), pltpu.roll(v, 1, 1))


def link(ref, mu, rows=3):
    return [[tuple(ref[(mu * 2 + c) * 9 + a * 3 + b] for c in range(2)) for b in range(3)] for a in range(rows)]


def spinor(ref, n, s, c):
    return tuple(ref[((n * 2 + k) * 4 + s) * 3 + c] for k in range(2))


def upper(ref, mu, sign, n, s, c):
    col, phase = BLOCKS[mu][s]
    return add_phase(spinor(ref, n, s, c), sign * phase, spinor(ref, n, 2 + col, c))


def half(ref, mu, sign):
    return {k: upper(ref, mu, sign, *k) for k in SPINS}


def flat_half(h):
    return [h[k][c] for k in SPINS for c in range(2)]


def unflat_half(flat):
    return {k: (flat[2 * i], flat[2 * i + 1]) for i, k in enumerate(SPINS)}


def apply(m, h):
    return {(n, s, a): csum([cmul(m[a][b], h[n, s, b]) for b in range(3)]) for n, s, a in SPINS}


def apply_dagger(m, h):
    return {(n, s, a): csum([cmulc(h[n, s, b], m[b][a]) for b in range(3)]) for n, s, a in SPINS}


def others(d):
    return [nu for nu in range(4) if nu != d]


def low_values(lref, xref, d):
    out = []
    for nu in others(d):
        m = link(lref, nu, 2)
        out += [m[a][b][c] for a, b in ROWS for c in range(2)]
    return out + flat_half(half(xref, d, -1))


def put(ref, at, flat):
    for i, v in enumerate(flat):
        ref[at + i] = v


def get(ref, at, n):
    return [ref[at + i] for i in range(n)]


def pack_kernel(flags, lref, xref, zd, zu, ta, tb, ra, rb, gref):
    sites = Sites()
    g = []
    for d in range(3):
        flat = flat_half(apply_dagger(link(lref, d), half(xref, d, 1)))
        put(gref, 24 * d, flat)
        g.append(flat)
    for d in (Z, T, R):
        low = low_values(lref, xref, d)
        low_out = [sites.pack_low(low[2 * i], low[2 * i + 1], d) for i in range(30)]
        high_out = [sites.pack_high(g[d][2 * i], g[d][2 * i + 1], d) for i in range(12)]
        if d == T:
            low_out = low_out[:18] + [jnp.where(flags[0] == 0, -v, v) for v in low_out[18:]]
            high_out = [jnp.where(flags[1] == 0, -v, v) for v in high_out]
        if d != T:
            put(zd if d == Z else ra, 0, low_out)
            put(zu if d == Z else rb, 0, high_out)
            continue
        swap_put(flags[2], (ta, tb), low_out, high_out)


def swap_put(even, refs, low, high):
    flag = even == 1
    for i in range(max(len(low), len(high))):
        a = low[i] if i < len(low) else high[i]
        b = high[i] if i < len(high) else low[i]
        refs[0][i] = jnp.where(flag, b, a)
        refs[1][i] = jnp.where(flag, a, b)


def swap_get(even, refs, n, low):
    flag = even == 1
    first, second = refs if low else (refs[1], refs[0])
    return [jnp.where(flag, first[i], second[i]) for i in range(n)]


def local_kernel(lref, xref, yref, wref, gyref, m2ref):
    sites = Sites()
    u = link(lref, Y)
    h = {k: tuple(sites.y_ahead(v) for v in c) for k, c in half(xref, Y, -1).items()}
    w = apply(u, h)
    g = {k: tuple(sites.y_behind(v) for v in c) for k, c in apply_dagger(u, half(xref, Y, 1)).items()}
    put(wref, 0, flat_half(w))
    put(gyref, 0, flat_half(g))
    for n in range(2):
        for s in range(2):
            for c in range(3):
                x = spinor(xref, n, s, c)
                store_spinor(yref, n, s, c, [x[i] - HOPPING * (w[n, s, c][i] + g[n, s, c][i]) for i in range(2)])
        for r in range(2):
            col, phase = BLOCKS[Y][r]
            for c in range(3):
                x = spinor(xref, n, 2 + col, c)
                diff = [g[n, r, c][i] - w[n, r, c][i] for i in range(2)]
                term = add_phase((0.0, 0.0), complex(phase).conjugate(), diff)
                store_spinor(yref, n, 2 + col, c, [x[i] - HOPPING * term[i] for i in range(2)])
    for mu in range(3):
        m = [[tuple(sites.y_ahead(v) for v in e) for e in row] for row in link(lref, mu)]
        m2 = matmul(u, m)
        put(m2ref, 18 * mu, [m2[a][b][c] for a in range(3) for b in range(3) for c in range(2)])


def store_spinor(ref, n, s, c, value):
    for k in range(2):
        ref[((n * 2 + k) * 4 + s) * 3 + c] = value[k]


def mat_at(ref, at):
    return [[(ref[at + (a * 3 + b) * 2], ref[at + (a * 3 + b) * 2 + 1]) for b in range(3)] for a in range(3)]


def put_mat(ref, at, m):
    put(ref, at, [m[a][b][c] for a in range(3) for b in range(3) for c in range(2)])


def middle_kernel(
    flags, lref, xref, gref, ylref, wyref, gyref, m2ref, zd, zu, ta, tb, ra, rb,
    ozu, ozd, ota, otb, ora, orb, oe, on, obase, oy, ow, nyref, fref, gsref,
):
    sites = Sites()
    put(oy, 0, get(ylref, 0, 48))
    put(ow, 72, get(wyref, 0, 24))
    slot = {}
    for d in range(3):
        if d != T:
            low_in, high_in = get(zd if d == Z else ra, 0, 30), get(zu if d == Z else rb, 0, 12)
        else:
            refs = (ta, tb) if d == T else (ra, rb)
            low_in = swap_get(flags[2 + d // 2], refs, 30, True)
            high_in = swap_get(flags[2 + d // 2], refs, 12, False)
        own = low_values(lref, xref, d)
        ahead = []
        for i in range(30):
            ahead += sites.ahead(own[2 * i], own[2 * i + 1], low_in[i], d)
        for k, nu in enumerate(others(d)):
            f = ahead[12 * k : 12 * k + 12]
            two = [[(f[(a * 3 + b) * 2], f[(a * 3 + b) * 2 + 1]) for b in range(3)] for a in range(2)]
            put_mat(fref, 18 * (3 * d + k), third_row(two))
            slot[d, nu] = 18 * (3 * d + k)
        own = get(gref, 24 * d, 24)
        behind = []
        for i in range(12):
            behind += sites.behind(own[2 * i], own[2 * i + 1], high_in[i], d)
        put(gsref, 24 * d, behind)
        g = unflat_half(behind)
        w = apply(link(lref, d), unflat_half(ahead[36:]))
        put(ow, 24 * d, flat_half(w))
        for n in range(2):
            for s in range(2):
                for c in range(3):
                    y = spinor(oy, n, s, c)
                    store_spinor(oy, n, s, c, [y[i] - HOPPING * (w[n, s, c][i] + g[n, s, c][i]) for i in range(2)])
            for r in range(2):
                col, phase = BLOCKS[d][r]
                for c in range(3):
                    y = spinor(oy, n, 2 + col, c)
                    diff = [HOPPING * (g[n, r, c][i] - w[n, r, c][i]) for i in range(2)]
                    y = add_phase(y, -complex(phase).conjugate(), diff)
                    store_spinor(oy, n, 2 + col, c, y)
    base = [[0.0] * 8 for _ in range(4)]
    lower = {}
    for mu in range(4):
        for nu in range(mu + 1, 4):
            u_mu, u_nu = link(lref, mu), link(lref, nu)
            m1 = matmul(u_mu, mat_at(fref, slot[mu, nu]))
            m2 = mat_at(m2ref, 18 * mu) if nu == Y else matmul(u_nu, mat_at(fref, slot[nu, mu]))
            p = antihermitian(matmul_dagger(m1, m2), PLAQUETTE)
            base[mu] = [a + b for a, b in zip(base[mu], p)]
            base[nu] = [a - b for a, b in zip(base[nu], p)]
            lower[mu, nu] = [-v for v in transport(p, u_nu)]
            lower[nu, mu] = transport(p, u_mu)
    for mu in range(3):
        moved = [sites.y_behind(v) for v in lower[mu, Y]]
        base[mu] = [a + b for a, b in zip(base[mu], moved)]
    for mu in range(4):
        put(obase, 8 * mu, base[mu])
    for d in range(4):
        g = unflat_half(get(gsref, 24 * d, 24) if d < 3 else get(gyref, 0, 24))
        k = half(oy, d, 1)
        m = [
            [csum([cmulc(k[n, s, a], g[n, s, b]) for n in range(2) for s in range(2)]) for b in range(3)]
            for a in range(3)
        ]
        part = antihermitian(m, HOPPING)
        if d == Y:
            put(nyref, 0, [sites.y_ahead(v) for v in part])
            continue
        put(on, 8 * d, part)
        low_out = [sites.pack_low(part[2 * i], part[2 * i + 1], d) for i in range(4)]
        up = []
        for mu in others(d):
            up += lower[mu, d]
        put(oe, 24 * d, up)
        high_out = [sites.pack_high(up[2 * i], up[2 * i + 1], d) for i in range(12)]
        if d != T:
            put(ozd if d == Z else ora, 0, low_out)
            put(ozu if d == Z else orb, 0, high_out)
        else:
            swap_put(flags[2 + d // 2], (ota, otb) if d == T else (ora, orb), low_out, high_out)


def inner_kernel(lref, yref, wref, nyref, baseref, oref):
    for mu in range(4):
        w = unflat_half(get(wref, 24 * mu, 24))
        k = half(yref, mu, -1)
        m = [
            [csum([cmulc(w[n, s, a], k[n, s, b]) for n in range(2) for s in range(2)]) for b in range(3)]
            for a in range(3)
        ]
        part = antihermitian(m, HOPPING)
        total = [a + b for a, b in zip(part, get(baseref, 8 * mu, 8))]
        if mu == Y:
            u = link(lref, Y)
            w_dagger = [[conj(u[j][a]) for j in range(3)] for a in range(3)]
            total = [a + b for a, b in zip(total, transport(get(nyref, 0, 8), w_dagger))]
        put(oref, 8 * mu, total)


def last_kernel(flags, lref, baseref, eref, nref, zu, zd, ta, tb, ra, rb, oref):
    sites = Sites()
    total = [get(baseref, 8 * mu, 8) for mu in range(4)]
    for d in range(3):
        if d != T:
            low_in, high_in = get(zd if d == Z else ra, 0, 4), get(zu if d == Z else rb, 0, 12)
        else:
            refs = (ta, tb) if d == T else (ra, rb)
            low_in = swap_get(flags[2 + d // 2], refs, 4, True)
            high_in = swap_get(flags[2 + d // 2], refs, 12, False)
        own = get(eref, 24 * d, 24)
        behind = []
        for i in range(12):
            behind += sites.behind(own[2 * i], own[2 * i + 1], high_in[i], d)
        for k, mu in enumerate(others(d)):
            total[mu] = [a + b for a, b in zip(total[mu], behind[8 * k : 8 * k + 8])]
        own = get(nref, 8 * d, 8)
        ahead = []
        for i in range(4):
            ahead += sites.ahead(own[2 * i], own[2 * i + 1], low_in[i], d)
        u = link(lref, d)
        w_dagger = [[conj(u[j][a]) for j in range(3)] for a in range(3)]
        total[d] = [a + b for a, b in zip(total[d], transport(ahead, w_dagger))]
    zero = jnp.zeros((4, 128), jnp.float32)
    for mu in range(4):
        x = total[mu]
        at = mu * 18
        for i, (a, b) in enumerate(OFF):
            oref[at + a * 3 + b] = x[2 * i]
            oref[at + b * 3 + a] = -x[2 * i]
            oref[at + 9 + a * 3 + b] = x[2 * i + 1]
            oref[at + 9 + b * 3 + a] = x[2 * i + 1]
        for a in range(3):
            oref[at + a * 4] = zero
        oref[at + 9] = x[6]
        oref[at + 13] = x[7]
        oref[at + 17] = -(x[6] + x[7])


def call(body, operands, outs, flops, scratch=()):
    specs = [
        pl.BlockSpec(memory_space=pltpu.SMEM if o.dtype == jnp.int32 else pltpu.VMEM) for o in operands
    ]
    return pl.pallas_call(
        body,
        in_specs=specs,
        out_specs=[pl.BlockSpec(memory_space=pltpu.VMEM) for _ in outs],
        out_shape=[jax.ShapeDtypeStruct((n, 4, 128), jnp.float32) for n in outs],
        scratch_shapes=[pltpu.VMEM((n, 4, 128), jnp.float32) for n in scratch],
        cost_estimate=pl.CostEstimate(flops=flops, bytes_accessed=4 * 512 * 200, transcendentals=0),
        compiler_params=pltpu.CompilerParams(vmem_limit_bytes=8 * 1024 * 1024),
        interpret=INTERPRET,
    )(*operands)


def move(x, axis, by):
    size = lax.axis_size(axis)
    return lax.ppermute(x, axis, [(i, (i + by) % size) for i in range(size)])


def meet(x, axis, first):
    size = lax.axis_size(axis)
    pairs = []
    for i in range(0 if first else 1, size, 2):
        j = (i + 1) % size
        pairs += [(i, j), (j, i)]
    return lax.ppermute(x, axis, pairs)


def exchange(zd, zu, ta, tb, ra, rb):
    moves = {
        "zd": lambda: move(zd, "gz", -1),
        "zu": lambda: move(zu, "gz", 1),
        "ta": lambda: meet(ta, "ta", True),
        "tb": lambda: meet(tb, "ta", False),
        "ra": lambda: move(ra, "xy", -1),
        "rb": lambda: move(rb, "xy", 1),
    }
    out = {}
    for name in moves:
        out[name] = moves[name]()
    return [out[name] for name in moves]


def on_device(links, solutions):
    shape = links.shape
    lk = links.reshape(72, 4, 128)
    xs = solutions.reshape(48, 4, 128)
    t, r = lax.axis_index("ta"), lax.axis_index("xy")
    flags = jnp.stack([t, lax.axis_size("ta") - 1 - t, 1 - t % 2, 1 - r % 2]).astype(jnp.int32)
    zd, zu, ta, tb, ra, rb, g = call(pack_kernel, (flags, lk, xs), (30, 12, 30, 30, 30, 12, 72), 4_000_000)
    zd, zu, ta, tb, ra, rb = exchange(zd, zu, ta, tb, ra, rb)
    yl, wy, gy, m2 = call(local_kernel, (lk, xs), (48, 24, 24, 54), 20_000_000)
    ozu, ozd, ota, otb, ora, orb, e, n, base, y, w, ny = call(
        middle_kernel,
        (flags, lk, xs, g, yl, wy, gy, m2, zd, zu, ta, tb, ra, rb),
        (12, 4, 12, 12, 4, 12, 72, 24, 32, 48, 96, 8),
        20_000_000,
        (162, 72),
    )
    ozd, ozu, ota, otb, ora, orb = exchange(ozd, ozu, ota, otb, ora, orb)
    (base,) = call(inner_kernel, (lk, y, w, ny, base), (32,), 20_000_000)
    (force,) = call(last_kernel, (flags, lk, base, e, n, ozu, ozd, ota, otb, ora, orb), (72,), 4_000_000)
    return force.reshape(shape)


def solution(mesh):
    spec = P(None, None, None, None, "ta", "gz", "xy")

    return jax.shard_map(on_device, mesh=mesh, in_specs=(spec, spec), out_specs=spec, check_vma=False)
```

```python
import jax
import jax.numpy as jnp
from jax import lax
from jax.experimental import pallas as pl
from jax.experimental.pallas import tpu as pltpu
from jax.sharding import PartitionSpec as P


HOPPING = 0.125
PLAQUETTE = 0.5
INTERPRET = False

BLOCKS = (
    ((0, 1), (1, 1)),
    ((0, 1j), (1, -1j)),
    ((1, 1j), (0, 1j)),
    ((1, -1), (0, 1)),
)
T, Z, R, Y = 0, 1, 2, 3
OFF = ((0, 1), (0, 2), (1, 2))
ROWS = tuple((a, b) for a in range(2) for b in range(3))
SPINS = tuple((n, s, c) for n in range(2) for s in range(2) for c in range(3))


def add_phase(a, phase, b):
    if phase == 1:
        return (a[0] + b[0], a[1] + b[1])
    if phase == -1:
        return (a[0] - b[0], a[1] - b[1])
    if phase == 1j:
        return (a[0] - b[1], a[1] + b[0])
    return (a[0] + b[1], a[1] - b[0])


def cmul(a, b):
    return (a[0] * b[0] - a[1] * b[1], a[0] * b[1] + a[1] * b[0])


def cmulc(a, b):
    return (a[0] * b[0] + a[1] * b[1], a[1] * b[0] - a[0] * b[1])


def conj(a):
    return (a[0], -a[1])


def csum(terms):
    re, im = terms[0]
    for t in terms[1:]:
        re, im = re + t[0], im + t[1]
    return (re, im)


def csub(a, b):
    return (a[0] - b[0], a[1] - b[1])


def matmul(left, right):
    return [[csum([cmul(left[a][k], right[k][b]) for k in range(3)]) for b in range(3)] for a in range(3)]


def matmul_dagger(left, right):
    return [[csum([cmulc(left[a][k], right[b][k]) for k in range(3)]) for b in range(3)] for a in range(3)]


def third_row(m):
    u, v = m
    cross = lambda i, j: conj(csub(cmul(u[i], v[j]), cmul(u[j], v[i])))
    return [u, v, [cross(1, 2), cross(2, 0), cross(0, 1)]]


def antihermitian(m, scale):
    out = []
    for a, b in OFF:
        out.append((0.5 * scale) * (m[a][b][0] - m[b][a][0]))
        out.append((0.5 * scale) * (m[a][b][1] + m[b][a][1]))
    third = (m[0][0][1] + m[1][1][1] + m[2][2][1]) * (1.0 / 3.0)
    out.append(scale * (m[0][0][1] - third))
    out.append(scale * (m[1][1][1] - third))
    return out


def transport(x, w):
    e = {}
    for i, (a, b) in enumerate(OFF):
        e[a, b] = (x[2 * i], x[2 * i + 1])
        e[b, a] = (-x[2 * i], x[2 * i + 1])
    d = (x[6], x[7], -(x[6] + x[7]))
    v = []
    for a in range(3):
        row = []
        for j in range(3):
            terms = [(-d[a] * w[a][j][1], d[a] * w[a][j][0])]
            terms += [cmul(e[a, b], w[b][j]) for b in range(3) if b != a]
            row.append(csum(terms))
        v.append(row)
    out = []
    for i, j in OFF:
        t = csum([cmulc(v[a][j], w[a][i]) for a in range(3)])
        out += [t[0], t[1]]
    for i in range(2):
        s = None
        for a in range(3):
            p = v[a][i][1] * w[a][i][0] - v[a][i][0] * w[a][i][1]
            s = p if s is None else s + p
        out.append(s)
    return out


class Sites:
    def __init__(self):
        rows = lax.broadcasted_iota(jnp.int32, (4, 128), 0)
        lanes = lax.broadcasted_iota(jnp.int32, (4, 128), 1)
        self.first = (rows < 2, rows % 2 == 0, lanes < 64)
        self.y_last = lanes % 64 == 63
        self.y_first = lanes % 64 == 0

    def swap(self, v, d):
        if d == R:
            return pltpu.roll(v, 64, 1)
        if d == T:
            return jnp.concatenate([v[2:4], v[0:2]], axis=0)
        return jnp.where(
            self.first[Z],
            jnp.concatenate([v[1:4], v[0:1]], axis=0),
            jnp.concatenate([v[3:4], v[0:3]], axis=0),
        )

    def pack_low(self, a, b, d):
        return jnp.where(self.first[d], a, self.swap(b, d))

    def pack_high(self, a, b, d):
        return jnp.where(self.first[d], self.swap(b, d), a)

    def ahead(self, a, b, m, d):
        return (
            self.swap(jnp.where(self.first[d], m, a), d),
            jnp.where(self.first[d], self.swap(b, d), m),
        )

    def behind(self, a, b, m, d):
        return (
            self.swap(jnp.where(self.first[d], a, m), d),
            jnp.where(self.first[d], m, self.swap(b, d)),
        )

    def y_ahead(self, v):
        return jnp.where(self.y_last, pltpu.roll(v, 63, 1), pltpu.roll(v, 127, 1))

    def y_behind(self, v):
        return jnp.where(self.y_first, pltpu.roll(v, 65, 1), pltpu.roll(v, 1, 1))


def link(ref, mu, rows=3):
    return [[tuple(ref[(mu * 2 + c) * 9 + a * 3 + b] for c in range(2)) for b in range(3)] for a in range(rows)]


def spinor(ref, n, s, c):
    return tuple(ref[((n * 2 + k) * 4 + s) * 3 + c] for k in range(2))


def upper(ref, mu, sign, n, s, c):
    col, phase = BLOCKS[mu][s]
    return add_phase(spinor(ref, n, s, c), sign * phase, spinor(ref, n, 2 + col, c))


def half(ref, mu, sign):
    return {k: upper(ref, mu, sign, *k) for k in SPINS}


def flat_half(h):
    return [h[k][c] for k in SPINS for c in range(2)]


def unflat_half(flat):
    return {k: (flat[2 * i], flat[2 * i + 1]) for i, k in enumerate(SPINS)}


def apply(m, h):
    return {(n, s, a): csum([cmul(m[a][b], h[n, s, b]) for b in range(3)]) for n, s, a in SPINS}


def apply_dagger(m, h):
    return {(n, s, a): csum([cmulc(h[n, s, b], m[b][a]) for b in range(3)]) for n, s, a in SPINS}


def others(d):
    return [nu for nu in range(4) if nu != d]


def row_values(lref, nus):
    out = []
    for nu in nus:
        m = link(lref, nu, 2)
        out += [m[a][b][c] for a, b in ROWS for c in range(2)]
    return out


def rows_of(flat):
    return [[(flat[(a * 3 + b) * 2], flat[(a * 3 + b) * 2 + 1]) for b in range(3)] for a in range(2)]


def put(ref, at, flat):
    for i, v in enumerate(flat):
        ref[at + i] = v


def get(ref, at, n):
    return [ref[at + i] for i in range(n)]


LOW_LINKS, LOW = 18, 30
HIGH_LINKS, HIGH = 24, 36
AGAIN = 16


def pack_kernel(flags, lref, xref, zd, zu, ta, tb, rd, ru, gref):
    sites = Sites()
    for d in (Z, T, R):
        g = flat_half(apply_dagger(link(lref, d), half(xref, d, 1)))
        put(gref, 24 * d, g)
        low = row_values(lref, others(d)) + flat_half(half(xref, d, -1))
        high = row_values(lref, range(4)) + g
        low = [sites.pack_low(low[2 * i], low[2 * i + 1], d) for i in range(LOW)]
        high = [sites.pack_high(high[2 * i], high[2 * i + 1], d) for i in range(HIGH)]
        if d != T:
            put(zd if d == Z else rd, 0, low)
            put(zu if d == Z else ru, 0, high)
            continue
        low = low[:LOW_LINKS] + [jnp.where(flags[0] == 0, -v, v) for v in low[LOW_LINKS:]]
        high = high[:HIGH_LINKS] + [jnp.where(flags[1] == 0, -v, v) for v in high[HIGH_LINKS:]]
        even = flags[2] == 1
        for i in range(HIGH):
            x = low[i] if i < LOW else high[i]
            ta[i] = jnp.where(even, high[i], x)
            tb[i] = jnp.where(even, x, high[i])


class Halo:
    def __init__(self, flags, zd, zu, ta, tb, rd, ru):
        self.even = flags[2] == 1
        self.refs = {Z: (zd, zu), T: (ta, tb), R: (rd, ru)}

    def low(self, d, i):
        first, second = self.refs[d]
        return jnp.where(self.even, first[i], second[i]) if d == T else first[i]

    def high(self, d, i):
        first, second = self.refs[d]
        return jnp.where(self.even, second[i], first[i]) if d == T else second[i]

    def ahead(self, sites, d, own, at):
        out = []
        for i in range(len(own) // 2):
            out += sites.ahead(own[2 * i], own[2 * i + 1], self.low(d, at + i), d)
        return out

    def behind(self, sites, d, own, at):
        out = []
        for i in range(len(own) // 2):
            out += sites.behind(own[2 * i], own[2 * i + 1], self.high(d, at + i), d)
        return out


def local_kernel(lref, xref, yref, wref, gyref, m2ref):
    sites = Sites()
    u = link(lref, Y)
    h = {k: tuple(sites.y_ahead(v) for v in c) for k, c in half(xref, Y, -1).items()}
    w = apply(u, h)
    g = {k: tuple(sites.y_behind(v) for v in c) for k, c in apply_dagger(u, half(xref, Y, 1)).items()}
    put(wref, 0, flat_half(w))
    put(gyref, 0, flat_half(g))
    for n in range(2):
        for s in range(2):
            for c in range(3):
                x = spinor(xref, n, s, c)
                store_spinor(yref, n, s, c, [x[i] - HOPPING * (w[n, s, c][i] + g[n, s, c][i]) for i in range(2)])
        for r in range(2):
            col, phase = BLOCKS[Y][r]
            for c in range(3):
                x = spinor(xref, n, 2 + col, c)
                diff = [g[n, r, c][i] - w[n, r, c][i] for i in range(2)]
                term = add_phase((0.0, 0.0), complex(phase).conjugate(), diff)
                store_spinor(yref, n, 2 + col, c, [x[i] - HOPPING * term[i] for i in range(2)])
    for mu in range(3):
        m = [[tuple(sites.y_ahead(v) for v in e) for e in row] for row in link(lref, mu)]
        m2 = matmul(u, m)
        put(m2ref, 18 * mu, [m2[a][b][c] for a in range(3) for b in range(3) for c in range(2)])


def store_spinor(ref, n, s, c, value):
    for k in range(2):
        ref[((n * 2 + k) * 4 + s) * 3 + c] = value[k]


def mat_at(ref, at):
    return [[(ref[at + (a * 3 + b) * 2], ref[at + (a * 3 + b) * 2 + 1]) for b in range(3)] for a in range(3)]


def put_mat(ref, at, m):
    put(ref, at, [m[a][b][c] for a in range(3) for b in range(3) for c in range(2)])


def add_hops(yref, d, w, g):
    for n in range(2):
        for s in range(2):
            for c in range(3):
                y = spinor(yref, n, s, c)
                store_spinor(yref, n, s, c, [y[i] - HOPPING * (w[n, s, c][i] + g[n, s, c][i]) for i in range(2)])
        for r in range(2):
            col, phase = BLOCKS[d][r]
            for c in range(3):
                diff = [HOPPING * (g[n, r, c][i] - w[n, r, c][i]) for i in range(2)]
                y = add_phase(spinor(yref, n, 2 + col, c), -complex(phase).conjugate(), diff)
                store_spinor(yref, n, 2 + col, c, y)


def outer(p, q):
    return [
        [csum([cmulc(p[n, s, a], q[n, s, b]) for n in range(2) for s in range(2)]) for b in range(3)]
        for a in range(3)
    ]


def partner_kernel(
    flags, lref, xref, gref, ylref, zd, zu, ta, tb, rd, ru,
    oz, ot, orow, oy, ow, on, ob,
):
    sites = Sites()
    halo = Halo(flags, zd, zu, ta, tb, rd, ru)
    put(oy, 0, get(ylref, 0, 48))
    kept = []
    for d in range(3):
        h = unflat_half(halo.ahead(sites, d, flat_half(half(xref, d, -1)), LOW_LINKS))
        g = unflat_half(halo.behind(sites, d, get(gref, 24 * d, 24), HIGH_LINKS))
        w = apply(link(lref, d), h)
        put(ow, 24 * d, flat_half(w))
        add_hops(oy, d, w, g)
        kept.append(g)
        put(ob, 12 * d, halo.behind(sites, d, row_values(lref, (d,)), 6 * d))
    for mu in (Z, T, R):
        part = antihermitian(outer(half(oy, mu, 1), kept[mu]), HOPPING)
        put(on, 8 * mu, part)
        moved = part + [v for d in range(3) if d != mu for v in get(ob, 12 * d, 12)]
        ref = {Z: oz, T: ot, R: orow}[mu]
        put(ref, 0, [sites.pack_low(moved[2 * i], moved[2 * i + 1], mu) for i in range(AGAIN)])


def adjoint(m):
    return [[conj(m[b][a]) for b in range(3)] for a in range(3)]


def gauge_kernel(
    flags, lref, yref, wref, wyref, gyref, m2ref, zd, zu, ta, tb, rd, ru, obase, oq, fref, bref,
):
    sites = Sites()
    halo = Halo(flags, zd, zu, ta, tb, rd, ru)
    slot = {}
    for d in range(3):
        flat = halo.ahead(sites, d, row_values(lref, others(d)), 0)
        for k, nu in enumerate(others(d)):
            slot[d, nu] = 18 * (3 * d + k)
            put_mat(fref, slot[d, nu], third_row(rows_of(flat[12 * k : 12 * k + 12])))
    base = [[0.0] * 8 for _ in range(4)]

    def add(mu, part):
        base[mu] = [a + b for a, b in zip(base[mu], part)]

    for mu in range(4):
        for nu in range(mu + 1, 4):
            m1 = matmul(link(lref, mu), mat_at(fref, slot[mu, nu]))
            m2 = mat_at(m2ref, 18 * mu) if nu == Y else matmul(link(lref, nu), mat_at(fref, slot[nu, mu]))
            p = antihermitian(matmul_dagger(m1, m2), PLAQUETTE)
            add(mu, p)
            add(nu, [-v for v in p])
            if nu == Y:
                add(mu, [-sites.y_behind(v) for v in transport(p, link(lref, Y))])
    for d in range(3):
        flat = halo.behind(sites, d, row_values(lref, range(4)), 0)
        for nu in range(4):
            put_mat(bref, 18 * nu, third_row(rows_of(flat[12 * nu : 12 * nu + 12])))
        b_d = mat_at(bref, 18 * d)
        slot_q = 0
        for mu in others(d):
            q = matmul(adjoint(mat_at(bref, 18 * mu)), b_d)
            if mu == Y:
                c = [[tuple(sites.y_ahead(v) for v in e) for e in row] for row in b_d]
                v = matmul(adjoint(c), q)
                add(Y, antihermitian(matmul(link(lref, Y), v), PLAQUETTE))
            else:
                put_mat(oq, 18 * (2 * d + slot_q), [[(PLAQUETTE * e[0], PLAQUETTE * e[1]) for e in row] for row in q])
                slot_q += 1
    for mu in range(4):
        w = unflat_half(get(wref, 24 * mu, 24) if mu != Y else get(wyref, 0, 24))
        add(mu, antihermitian(outer(w, half(yref, mu, -1)), HOPPING))
    part = antihermitian(outer(half(yref, Y, 1), unflat_half(get(gyref, 0, 24))), HOPPING)
    add(Y, transport([sites.y_ahead(v) for v in part], adjoint(link(lref, Y))))
    for mu in range(4):
        put(obase, 8 * mu, base[mu])


def times_dagger(x, u):
    e = {}
    for i, (a, b) in enumerate(OFF):
        e[a, b] = (x[2 * i], x[2 * i + 1])
        e[b, a] = (-x[2 * i], x[2 * i + 1])
    d = (x[6], x[7], -(x[6] + x[7]))
    return [
        [
            csum([(d[a] * u[j][a][1], d[a] * u[j][a][0])] + [cmulc(e[a, b], u[j][b]) for b in range(3) if b != a])
            for j in range(3)
        ]
        for a in range(3)
    ]


def last_kernel(lref, baseref, nref, bref, qref, zd, td, rd, oref):
    sites = Sites()
    zero = jnp.zeros((4, 128), jnp.float32)
    for mu in range(4):
        x = get(baseref, 8 * mu, 8)
        if mu != Y:
            m = {Z: zd, T: td, R: rd}[mu]
            others_of = [d for d in range(3) if d != mu]
            own = get(nref, 8 * mu, 8) + [v for d in others_of for v in get(bref, 12 * d, 12)]
            ahead = []
            for i in range(AGAIN):
                ahead += sites.ahead(own[2 * i], own[2 * i + 1], m[i], mu)
            u = link(lref, mu)
            total = times_dagger(ahead[:8], u)
            for k, d in enumerate(others_of):
                c = third_row(rows_of(ahead[8 + 12 * k : 20 + 12 * k]))
                slot_q = [e for e in others(d)].index(mu)
                v = matmul(adjoint(c), mat_at(qref, 18 * (2 * d + slot_q)))
                total = [[csum([total[a][b], v[a][b]]) for b in range(3)] for a in range(3)]
            x = [p + q for p, q in zip(x, antihermitian(matmul(u, total), 1.0))]
        at = mu * 18
        for i, (a, b) in enumerate(OFF):
            oref[at + a * 3 + b] = x[2 * i]
            oref[at + b * 3 + a] = -x[2 * i]
            oref[at + 9 + a * 3 + b] = x[2 * i + 1]
            oref[at + 9 + b * 3 + a] = x[2 * i + 1]
        for a in range(3):
            oref[at + a * 4] = zero
        oref[at + 9] = x[6]
        oref[at + 13] = x[7]
        oref[at + 17] = -(x[6] + x[7])


def call(body, operands, outs, flops, scratch=()):
    specs = [
        pl.BlockSpec(memory_space=pltpu.SMEM if o.dtype == jnp.int32 else pltpu.VMEM) for o in operands
    ]
    return pl.pallas_call(
        body,
        in_specs=specs,
        out_specs=[pl.BlockSpec(memory_space=pltpu.VMEM) for _ in outs],
        out_shape=[jax.ShapeDtypeStruct((n, 4, 128), jnp.float32) for n in outs],
        scratch_shapes=[pltpu.VMEM((n, 4, 128), jnp.float32) for n in scratch],
        cost_estimate=pl.CostEstimate(flops=flops, bytes_accessed=4 * 512 * 200, transcendentals=0),
        compiler_params=pltpu.CompilerParams(vmem_limit_bytes=8 * 1024 * 1024),
        interpret=INTERPRET,
    )(*operands)


def move(x, axis, by):
    size = lax.axis_size(axis)
    return lax.ppermute(x, axis, [(i, (i + by) % size) for i in range(size)])


def meet(x, axis, first):
    size = lax.axis_size(axis)
    pairs = []
    for i in range(0 if first else 1, size, 2):
        j = (i + 1) % size
        pairs += [(i, j), (j, i)]
    return lax.ppermute(x, axis, pairs)


def on_device(links, solutions):
    shape = links.shape
    lk = links.reshape(72, 4, 128)
    xs = solutions.reshape(48, 4, 128)
    t = lax.axis_index("ta")
    flags = jnp.stack([t, lax.axis_size("ta") - 1 - t, 1 - t % 2]).astype(jnp.int32)
    zd, zu, ta, tb, rd, ru, g = call(pack_kernel, (flags, lk, xs), (LOW, HIGH, HIGH, HIGH, LOW, HIGH, 72), 4_000_000)
    zu = move(zu, "gz", 1)
    zd = move(zd, "gz", -1)
    tb = meet(tb, "ta", False)
    ta = meet(ta, "ta", True)
    rd = move(rd, "xy", -1)
    ru = move(ru, "xy", 1)
    got = (zd, zu, ta, tb, rd, ru)
    yl, wy, gy, m2 = call(local_kernel, (lk, xs), (48, 24, 24, 54), 20_000_000)
    oz, ot, orow, y, w, n, b = call(
        partner_kernel, (flags, lk, xs, g, yl, *got), (AGAIN, AGAIN, AGAIN, 48, 72, 24, 36), 20_000_000
    )
    oz = move(oz, "gz", -1)
    ot = move(ot, "ta", -1)
    orow = move(orow, "xy", -1)
    base, q = call(gauge_kernel, (flags, lk, y, w, wy, gy, m2, *got), (32, 108), 20_000_000, (162, 72))
    (force,) = call(last_kernel, (lk, base, n, b, q, oz, ot, orow), (72,), 4_000_000)
    return force.reshape(shape)


def solution(mesh):
    spec = P(None, None, None, None, "ta", "gz", "xy")

    return jax.shard_map(on_device, mesh=mesh, in_specs=(spec, spec), out_specs=spec, check_vma=False)
```

```python
import jax
import jax.numpy as jnp
from jax import lax
from jax.experimental import pallas as pl
from jax.experimental.pallas import tpu as pltpu
from jax.sharding import PartitionSpec as P


HOPPING = 0.125
PLAQUETTE = 0.5
INTERPRET = False

BLOCKS = (
    ((0, 1), (1, 1)),
    ((0, 1j), (1, -1j)),
    ((1, 1j), (0, 1j)),
    ((1, -1), (0, 1)),
)
T, Z, R, Y = 0, 1, 2, 3
OFF = ((0, 1), (0, 2), (1, 2))
ROWS = tuple((a, b) for a in range(2) for b in range(3))
SPINS = tuple((n, s, c) for n in range(2) for s in range(2) for c in range(3))


def add_phase(a, phase, b):
    if phase == 1:
        return (a[0] + b[0], a[1] + b[1])
    if phase == -1:
        return (a[0] - b[0], a[1] - b[1])
    if phase == 1j:
        return (a[0] - b[1], a[1] + b[0])
    return (a[0] + b[1], a[1] - b[0])


def cmul(a, b):
    return (a[0] * b[0] - a[1] * b[1], a[0] * b[1] + a[1] * b[0])


def cmulc(a, b):
    return (a[0] * b[0] + a[1] * b[1], a[1] * b[0] - a[0] * b[1])


def conj(a):
    return (a[0], -a[1])


def csum(terms):
    re, im = terms[0]
    for t in terms[1:]:
        re, im = re + t[0], im + t[1]
    return (re, im)


def csub(a, b):
    return (a[0] - b[0], a[1] - b[1])


def matmul(left, right):
    return [[csum([cmul(left[a][k], right[k][b]) for k in range(3)]) for b in range(3)] for a in range(3)]


def matmul_dagger(left, right):
    return [[csum([cmulc(left[a][k], right[b][k]) for k in range(3)]) for b in range(3)] for a in range(3)]


def third_row(m):
    u, v = m
    cross = lambda i, j: conj(csub(cmul(u[i], v[j]), cmul(u[j], v[i])))
    return [u, v, [cross(1, 2), cross(2, 0), cross(0, 1)]]


def antihermitian(m, scale):
    out = []
    for a, b in OFF:
        out.append((0.5 * scale) * (m[a][b][0] - m[b][a][0]))
        out.append((0.5 * scale) * (m[a][b][1] + m[b][a][1]))
    third = (m[0][0][1] + m[1][1][1] + m[2][2][1]) * (1.0 / 3.0)
    out.append(scale * (m[0][0][1] - third))
    out.append(scale * (m[1][1][1] - third))
    return out


def transport(x, w):
    e = {}
    for i, (a, b) in enumerate(OFF):
        e[a, b] = (x[2 * i], x[2 * i + 1])
        e[b, a] = (-x[2 * i], x[2 * i + 1])
    d = (x[6], x[7], -(x[6] + x[7]))
    v = []
    for a in range(3):
        row = []
        for j in range(3):
            terms = [(-d[a] * w[a][j][1], d[a] * w[a][j][0])]
            terms += [cmul(e[a, b], w[b][j]) for b in range(3) if b != a]
            row.append(csum(terms))
        v.append(row)
    out = []
    for i, j in OFF:
        t = csum([cmulc(v[a][j], w[a][i]) for a in range(3)])
        out += [t[0], t[1]]
    for i in range(2):
        s = None
        for a in range(3):
            p = v[a][i][1] * w[a][i][0] - v[a][i][0] * w[a][i][1]
            s = p if s is None else s + p
        out.append(s)
    return out


class Sites:
    def __init__(self):
        rows = lax.broadcasted_iota(jnp.int32, (4, 128), 0)
        lanes = lax.broadcasted_iota(jnp.int32, (4, 128), 1)
        self.first = (rows < 2, rows % 2 == 0, lanes < 64)
        self.y_last = lanes % 64 == 63
        self.y_first = lanes % 64 == 0

    def swap(self, v, d):
        if d == R:
            return pltpu.roll(v, 64, 1)
        if d == T:
            return jnp.concatenate([v[2:4], v[0:2]], axis=0)
        return jnp.where(
            self.first[Z],
            jnp.concatenate([v[1:4], v[0:1]], axis=0),
            jnp.concatenate([v[3:4], v[0:3]], axis=0),
        )

    def pack_low(self, a, b, d):
        return jnp.where(self.first[d], a, self.swap(b, d))

    def pack_high(self, a, b, d):
        return jnp.where(self.first[d], self.swap(b, d), a)

    def ahead(self, a, b, m, d):
        return (
            self.swap(jnp.where(self.first[d], m, a), d),
            jnp.where(self.first[d], self.swap(b, d), m),
        )

    def behind(self, a, b, m, d):
        return (
            self.swap(jnp.where(self.first[d], a, m), d),
            jnp.where(self.first[d], m, self.swap(b, d)),
        )

    def y_ahead(self, v):
        return jnp.where(self.y_last, pltpu.roll(v, 63, 1), pltpu.roll(v, 127, 1))

    def y_behind(self, v):
        return jnp.where(self.y_first, pltpu.roll(v, 65, 1), pltpu.roll(v, 1, 1))


def link(ref, mu, rows=3):
    return [[tuple(ref[(mu * 2 + c) * 9 + a * 3 + b] for c in range(2)) for b in range(3)] for a in range(rows)]


def spinor(ref, n, s, c):
    return tuple(ref[((n * 2 + k) * 4 + s) * 3 + c] for k in range(2))


def upper(ref, mu, sign, n, s, c):
    col, phase = BLOCKS[mu][s]
    return add_phase(spinor(ref, n, s, c), sign * phase, spinor(ref, n, 2 + col, c))


def half(ref, mu, sign):
    return {k: upper(ref, mu, sign, *k) for k in SPINS}


def flat_half(h):
    return [h[k][c] for k in SPINS for c in range(2)]


def unflat_half(flat):
    return {k: (flat[2 * i], flat[2 * i + 1]) for i, k in enumerate(SPINS)}


def apply(m, h):
    return {(n, s, a): csum([cmul(m[a][b], h[n, s, b]) for b in range(3)]) for n, s, a in SPINS}


def apply_dagger(m, h):
    return {(n, s, a): csum([cmulc(h[n, s, b], m[b][a]) for b in range(3)]) for n, s, a in SPINS}


def others(d):
    return [nu for nu in range(4) if nu != d]


def row_values(lref, nus):
    out = []
    for nu in nus:
        m = link(lref, nu, 2)
        out += [m[a][b][c] for a, b in ROWS for c in range(2)]
    return out


def rows_of(flat):
    return [[(flat[(a * 3 + b) * 2], flat[(a * 3 + b) * 2 + 1]) for b in range(3)] for a in range(2)]


def put(ref, at, flat):
    for i, v in enumerate(flat):
        ref[at + i] = v


def get(ref, at, n):
    return [ref[at + i] for i in range(n)]


LOW_LINKS, LOW = 18, 30
HIGH_LINKS, HIGH = 24, 36
AGAIN = 16


def pack_kernel(flags, lhbm, xhbm, zd, zu, ta, tb, rd, ru, gref, lref, xref, sems):
    copies = [
        pltpu.make_async_copy(xhbm, xref, sems.at[0]),
        pltpu.make_async_copy(lhbm, lref, sems.at[1]),
    ]
    for c in copies:
        c.start()
    sites = Sites()
    for c in copies:
        c.wait()
    for d in (Z, T, R):
        g = flat_half(apply_dagger(link(lref, d), half(xref, d, 1)))
        put(gref, 24 * d, g)
        low = row_values(lref, others(d)) + flat_half(half(xref, d, -1))
        high = row_values(lref, range(4)) + g
        low = [sites.pack_low(low[2 * i], low[2 * i + 1], d) for i in range(LOW)]
        high = [sites.pack_high(high[2 * i], high[2 * i + 1], d) for i in range(HIGH)]
        if d != T:
            put(zd if d == Z else rd, 0, low)
            put(zu if d == Z else ru, 0, high)
            continue
        low = low[:LOW_LINKS] + [jnp.where(flags[0] == 0, -v, v) for v in low[LOW_LINKS:]]
        high = high[:HIGH_LINKS] + [jnp.where(flags[1] == 0, -v, v) for v in high[HIGH_LINKS:]]
        even = flags[2] == 1
        for i in range(HIGH):
            x = low[i] if i < LOW else high[i]
            ta[i] = jnp.where(even, high[i], x)
            tb[i] = jnp.where(even, x, high[i])


class Halo:
    def __init__(self, flags, zd, zu, ta, tb, rd, ru):
        self.even = None if flags is None else flags[2] == 1
        self.refs = {Z: (zd, zu), T: (ta, tb), R: (rd, ru)}

    def low(self, d, i):
        first, second = self.refs[d]
        return jnp.where(self.even, first[i], second[i]) if d == T else first[i]

    def high(self, d, i):
        first, second = self.refs[d]
        return jnp.where(self.even, second[i], first[i]) if d == T else second[i]

    def ahead(self, sites, d, own, at):
        out = []
        for i in range(len(own) // 2):
            out += sites.ahead(own[2 * i], own[2 * i + 1], self.low(d, at + i), d)
        return out

    def behind(self, sites, d, own, at):
        out = []
        for i in range(len(own) // 2):
            out += sites.behind(own[2 * i], own[2 * i + 1], self.high(d, at + i), d)
        return out


def store_spinor(ref, n, s, c, value):
    for k in range(2):
        ref[((n * 2 + k) * 4 + s) * 3 + c] = value[k]


def mat_at(ref, at):
    return [[(ref[at + (a * 3 + b) * 2], ref[at + (a * 3 + b) * 2 + 1]) for b in range(3)] for a in range(3)]


def put_mat(ref, at, m):
    put(ref, at, [m[a][b][c] for a in range(3) for b in range(3) for c in range(2)])


def add_hops(yref, d, w, g):
    for n in range(2):
        for s in range(2):
            for c in range(3):
                y = spinor(yref, n, s, c)
                store_spinor(yref, n, s, c, [y[i] - HOPPING * (w[n, s, c][i] + g[n, s, c][i]) for i in range(2)])
        for r in range(2):
            col, phase = BLOCKS[d][r]
            for c in range(3):
                diff = [HOPPING * (g[n, r, c][i] - w[n, r, c][i]) for i in range(2)]
                y = add_phase(spinor(yref, n, 2 + col, c), -complex(phase).conjugate(), diff)
                store_spinor(yref, n, 2 + col, c, y)


def outer(p, q):
    return [
        [csum([cmulc(p[n, s, a], q[n, s, b]) for n in range(2) for s in range(2)]) for b in range(3)]
        for a in range(3)
    ]


def adjoint(m):
    return [[conj(m[b][a]) for b in range(3)] for a in range(3)]


def su3(left, right):
    return third_row([[csum([cmul(left[a][k], right[k][b]) for k in range(3)]) for b in range(3)] for a in range(2)])


def y_ahead(sites, m):
    return [[tuple(sites.y_ahead(v) for v in e) for e in row] for row in m]


def lower_y(sites, u_y, b_d, b_y):
    return antihermitian(matmul(u_y, su3(adjoint(y_ahead(sites, b_d)), su3(adjoint(b_y), b_d))), PLAQUETTE)


def scaled(m):
    return [[(PLAQUETTE * e[0], PLAQUETTE * e[1]) for e in row] for row in m]


def plane(sites, base, mu, nu, m1, m2, u_y):
    def add(at, part):
        base[at] = [a + b for a, b in zip(base[at], part)]

    p = antihermitian(matmul_dagger(m1, m2), PLAQUETTE)
    add(mu, p)
    add(nu, [-v for v in p])
    if nu == Y:
        add(mu, [-sites.y_behind(v) for v in transport(p, u_y)])


def early_kernel(lref, xref, gref, rd, ru, oy, ow, og, ob, om2, of, oq, obase):
    sites = Sites()
    halo = Halo(None, None, None, None, None, rd, ru)
    u = link(lref, Y)
    put(oy, 0, [xref[i] for i in range(48)])
    h = {k: tuple(sites.y_ahead(v) for v in c) for k, c in half(xref, Y, -1).items()}
    w = apply(u, h)
    g = {k: tuple(sites.y_behind(v) for v in c) for k, c in apply_dagger(u, half(xref, Y, 1)).items()}
    put(ow, 24, flat_half(w))
    put(og, 24, flat_half(g))
    add_hops(oy, Y, w, g)
    for mu in (T, Z):
        put_mat(om2, 18 * mu, su3(u, y_ahead(sites, link(lref, mu))))
    h = unflat_half(halo.ahead(sites, R, flat_half(half(xref, R, -1)), LOW_LINKS))
    g = unflat_half(halo.behind(sites, R, get(gref, 24 * R, 24), HIGH_LINKS))
    w = apply(link(lref, R), h)
    put(ow, 0, flat_half(w))
    put(og, 0, flat_half(g))
    add_hops(oy, R, w, g)
    flat = halo.ahead(sites, R, row_values(lref, others(R)), 0)
    f = [third_row(rows_of(flat[12 * k : 12 * k + 12])) for k in range(3)]
    put_mat(of, 0, f[0])
    put_mat(of, 18, f[1])
    base = [[0.0] * 8 for _ in range(4)]
    plane(sites, base, R, Y, su3(link(lref, R), f[2]), su3(u, y_ahead(sites, link(lref, R))), u)
    flat = halo.behind(sites, R, row_values(lref, range(4)), 0)
    put(ob, 0, flat[12 * R : 12 * R + 12])
    b = [third_row(rows_of(flat[12 * nu : 12 * nu + 12])) for nu in range(4)]
    for k in (T, Z):
        put_mat(oq, 18 * k, scaled(su3(adjoint(b[k]), b[R])))
    low = lower_y(sites, u, b[R], b[Y])
    put(obase, 0, base[R])
    put(obase, 8, [p + q for p, q in zip(base[Y], low)])


def partner_kernel(
    flags, lref, xref, gref, ylref, gxref, bxref, zd, zu, ta, tb,
    oz, ot, orow, oy, ow, on, ob,
):
    sites = Sites()
    halo = Halo(flags, zd, zu, ta, tb, None, None)
    put(oy, 0, get(ylref, 0, 48))
    kept = {R: unflat_half(get(gxref, 0, 24))}
    rows = {R: get(bxref, 0, 12)}
    for d in (T, Z):
        h = unflat_half(halo.ahead(sites, d, flat_half(half(xref, d, -1)), LOW_LINKS))
        g = unflat_half(halo.behind(sites, d, get(gref, 24 * d, 24), HIGH_LINKS))
        w = apply(link(lref, d), h)
        put(ow, 24 * d, flat_half(w))
        add_hops(oy, d, w, g)
        kept[d] = g
        rows[d] = halo.behind(sites, d, row_values(lref, (d,)), 6 * d)
        put(ob, 12 * d, rows[d])
    for mu in (Z, T, R):
        part = antihermitian(outer(half(oy, mu, 1), kept[mu]), HOPPING)
        put(on, 8 * mu, part)
        moved = part + [v for d in range(3) if d != mu for v in rows[d]]
        ref = {Z: oz, T: ot, R: orow}[mu]
        put(ref, 0, [sites.pack_low(moved[2 * i], moved[2 * i + 1], mu) for i in range(AGAIN)])


def gauge_kernel(
    flags, lref, yref, wref, wxyref, gxyref, m2ref, fxref, bxyref, zd, zu, ta, tb, obase, oq, fref, bref,
):
    sites = Sites()
    halo = Halo(flags, zd, zu, ta, tb, None, None)
    slot = {}
    for d in (T, Z):
        flat = halo.ahead(sites, d, row_values(lref, others(d)), 0)
        for k, nu in enumerate(others(d)):
            slot[d, nu] = 18 * (3 * d + k)
            put_mat(fref, slot[d, nu], third_row(rows_of(flat[12 * k : 12 * k + 12])))
    base = [[0.0] * 8, [0.0] * 8, get(bxyref, 0, 8), get(bxyref, 8, 8)]

    def add(mu, part):
        base[mu] = [a + b for a, b in zip(base[mu], part)]

    for mu in (T, Z):
        for nu in range(mu + 1, 4):
            m1 = su3(link(lref, mu), mat_at(fref, slot[mu, nu]))
            if nu == Y:
                m2 = mat_at(m2ref, 18 * mu)
            else:
                m2 = su3(link(lref, nu), mat_at(fxref, 18 * mu) if nu == R else mat_at(fref, slot[nu, mu]))
            plane(sites, base, mu, nu, m1, m2, link(lref, Y))
    for d in (T, Z):
        flat = halo.behind(sites, d, row_values(lref, range(4)), 0)
        for nu in range(4):
            put_mat(bref, 18 * nu, third_row(rows_of(flat[12 * nu : 12 * nu + 12])))
        b_d = mat_at(bref, 18 * d)
        for k, mu in enumerate([e for e in range(3) if e != d]):
            put_mat(oq, 18 * (2 * d + k), scaled(su3(adjoint(mat_at(bref, 18 * mu)), b_d)))
        add(Y, lower_y(sites, link(lref, Y), b_d, mat_at(bref, 18 * Y)))
    for mu in range(4):
        w = unflat_half(get(wref, 24 * mu, 24) if mu < R else get(wxyref, 24 * (mu - R), 24))
        add(mu, antihermitian(outer(w, half(yref, mu, -1)), HOPPING))
    part = antihermitian(outer(half(yref, Y, 1), unflat_half(get(gxyref, 24, 24))), HOPPING)
    add(Y, transport([sites.y_ahead(v) for v in part], adjoint(link(lref, Y))))
    for mu in range(4):
        put(obase, 8 * mu, base[mu])


def times_dagger(x, u):
    e = {}
    for i, (a, b) in enumerate(OFF):
        e[a, b] = (x[2 * i], x[2 * i + 1])
        e[b, a] = (-x[2 * i], x[2 * i + 1])
    d = (x[6], x[7], -(x[6] + x[7]))
    return [
        [
            csum([(d[a] * u[j][a][1], d[a] * u[j][a][0])] + [cmulc(e[a, b], u[j][b]) for b in range(3) if b != a])
            for j in range(3)
        ]
        for a in range(3)
    ]


def last_kernel(lref, baseref, nref, bref, bxref, qref, qxref, zd, td, rd, oref):
    sites = Sites()
    zero = jnp.zeros((4, 128), jnp.float32)
    for mu in range(4):
        x = get(baseref, 8 * mu, 8)
        if mu != Y:
            m = {Z: zd, T: td, R: rd}[mu]
            others_of = [d for d in range(3) if d != mu]
            own = get(nref, 8 * mu, 8) + [v for d in others_of for v in (get(bxref, 0, 12) if d == R else get(bref, 12 * d, 12))]
            ahead = []
            for i in range(AGAIN):
                ahead += sites.ahead(own[2 * i], own[2 * i + 1], m[i], mu)
            u = link(lref, mu)
            total = times_dagger(ahead[:8], u)
            for k, d in enumerate(others_of):
                c = third_row(rows_of(ahead[8 + 12 * k : 20 + 12 * k]))
                q = mat_at(qxref, 18 * mu) if d == R else mat_at(qref, 18 * (2 * d + [e for e in range(3) if e != d].index(mu)))
                v = matmul(adjoint(c), q)
                total = [[csum([total[a][b], v[a][b]]) for b in range(3)] for a in range(3)]
            x = [p + q for p, q in zip(x, antihermitian(matmul(u, total), 1.0))]
        at = mu * 18
        for i, (a, b) in enumerate(OFF):
            oref[at + a * 3 + b] = x[2 * i]
            oref[at + b * 3 + a] = -x[2 * i]
            oref[at + 9 + a * 3 + b] = x[2 * i + 1]
            oref[at + 9 + b * 3 + a] = x[2 * i + 1]
        for a in range(3):
            oref[at + a * 4] = zero
        oref[at + 9] = x[6]
        oref[at + 13] = x[7]
        oref[at + 17] = -(x[6] + x[7])


def call(body, operands, outs, flops, scratch=(), hbm=(), sems=0):
    specs = [
        pl.BlockSpec(
            memory_space=pltpu.SMEM if o.dtype == jnp.int32 else pltpu.HBM if i in hbm else pltpu.VMEM
        )
        for i, o in enumerate(operands)
    ]
    scratch = [pltpu.VMEM((n, 4, 128), jnp.float32) for n in scratch]
    return pl.pallas_call(
        body,
        in_specs=specs,
        out_specs=[pl.BlockSpec(memory_space=pltpu.VMEM) for _ in outs],
        out_shape=[jax.ShapeDtypeStruct((n, 4, 128), jnp.float32) for n in outs],
        scratch_shapes=scratch + ([pltpu.SemaphoreType.DMA((sems,))] if sems else []),
        cost_estimate=pl.CostEstimate(flops=flops, bytes_accessed=4 * 512 * 200, transcendentals=0),
        compiler_params=pltpu.CompilerParams(vmem_limit_bytes=8 * 1024 * 1024),
        interpret=INTERPRET,
    )(*operands)


def move(x, axis, by):
    size = lax.axis_size(axis)
    return lax.ppermute(x, axis, [(i, (i + by) % size) for i in range(size)])


def meet(x, axis, first):
    size = lax.axis_size(axis)
    pairs = []
    for i in range(0 if first else 1, size, 2):
        j = (i + 1) % size
        pairs += [(i, j), (j, i)]
    return lax.ppermute(x, axis, pairs)


def on_device(links, solutions):
    shape = links.shape
    lk = links.reshape(72, 4, 128)
    xs = solutions.reshape(48, 4, 128)
    t = lax.axis_index("ta")
    flags = jnp.stack([t, lax.axis_size("ta") - 1 - t, 1 - t % 2]).astype(jnp.int32)
    zd, zu, ta, tb, rd, ru, g, lk, xs = call(
        pack_kernel,
        (flags, pltpu.with_memory_space_constraint(lk, pltpu.HBM), pltpu.with_memory_space_constraint(xs, pltpu.HBM)),
        (LOW, HIGH, HIGH, HIGH, LOW, HIGH, 72, 72, 48),
        4_000_000,
        hbm=(1, 2),
        sems=2,
    )
    zu = move(zu, "gz", 1)
    zd = move(zd, "gz", -1)
    tb = meet(tb, "ta", False)
    ta = meet(ta, "ta", True)
    rd = move(rd, "xy", -1)
    ru = move(ru, "xy", 1)
    got = (zd, zu, ta, tb)
    yl, wxy, gxy, bx, m2, fx, qx, bxy = call(
        early_kernel, (lk, xs, g, rd, ru), (48, 48, 48, 12, 36, 36, 36, 16), 20_000_000
    )
    oz, ot, orow, y, w, n, b = call(
        partner_kernel, (flags, lk, xs, g, yl, gxy, bx, *got), (AGAIN, AGAIN, AGAIN, 48, 48, 24, 24), 20_000_000
    )
    oz = move(oz, "gz", -1)
    ot = move(ot, "ta", -1)
    orow = move(orow, "xy", -1)
    base, q = call(gauge_kernel, (flags, lk, y, w, wxy, gxy, m2, fx, bxy, *got), (32, 72), 20_000_000, (108, 72))
    (force,) = call(last_kernel, (lk, base, n, b, bx, q, qx, oz, ot, orow), (72,), 4_000_000)
    return force.reshape(shape)


def solution(mesh):
    spec = P(None, None, None, None, "ta", "gz", "xy")

    return jax.shard_map(on_device, mesh=mesh, in_specs=(spec, spec), out_specs=spec, check_vma=False)
```

```python
import jax
import jax.numpy as jnp
from jax import lax
from jax.experimental import pallas as pl
from jax.experimental.pallas import tpu as pltpu
from jax.sharding import PartitionSpec as P


HOPPING = 0.125
PLAQUETTE = 0.5
INTERPRET = False

BLOCKS = (
    ((0, 1), (1, 1)),
    ((0, 1j), (1, -1j)),
    ((1, 1j), (0, 1j)),
    ((1, -1), (0, 1)),
)
T, Z, R, Y = 0, 1, 2, 3
OFF = ((0, 1), (0, 2), (1, 2))
ROWS = tuple((a, b) for a in range(2) for b in range(3))
SPINS = tuple((n, s, c) for n in range(2) for s in range(2) for c in range(3))


def add_phase(a, phase, b):
    if phase == 1:
        return (a[0] + b[0], a[1] + b[1])
    if phase == -1:
        return (a[0] - b[0], a[1] - b[1])
    if phase == 1j:
        return (a[0] - b[1], a[1] + b[0])
    return (a[0] + b[1], a[1] - b[0])


def cmul(a, b):
    return (a[0] * b[0] - a[1] * b[1], a[0] * b[1] + a[1] * b[0])


def cmulc(a, b):
    return (a[0] * b[0] + a[1] * b[1], a[1] * b[0] - a[0] * b[1])


def conj(a):
    return (a[0], -a[1])


def csum(terms):
    re, im = terms[0]
    for t in terms[1:]:
        re, im = re + t[0], im + t[1]
    return (re, im)


def csub(a, b):
    return (a[0] - b[0], a[1] - b[1])


def matmul(left, right):
    return [[csum([cmul(left[a][k], right[k][b]) for k in range(3)]) for b in range(3)] for a in range(3)]


def matmul_dagger(left, right):
    return [[csum([cmulc(left[a][k], right[b][k]) for k in range(3)]) for b in range(3)] for a in range(3)]


def third_row(m):
    u, v = m
    cross = lambda i, j: conj(csub(cmul(u[i], v[j]), cmul(u[j], v[i])))
    return [u, v, [cross(1, 2), cross(2, 0), cross(0, 1)]]


def antihermitian(m, scale):
    out = []
    for a, b in OFF:
        out.append((0.5 * scale) * (m[a][b][0] - m[b][a][0]))
        out.append((0.5 * scale) * (m[a][b][1] + m[b][a][1]))
    third = (m[0][0][1] + m[1][1][1] + m[2][2][1]) * (1.0 / 3.0)
    out.append(scale * (m[0][0][1] - third))
    out.append(scale * (m[1][1][1] - third))
    return out


def transport(x, w):
    e = {}
    for i, (a, b) in enumerate(OFF):
        e[a, b] = (x[2 * i], x[2 * i + 1])
        e[b, a] = (-x[2 * i], x[2 * i + 1])
    d = (x[6], x[7], -(x[6] + x[7]))
    v = []
    for a in range(3):
        row = []
        for j in range(3):
            terms = [(-d[a] * w[a][j][1], d[a] * w[a][j][0])]
            terms += [cmul(e[a, b], w[b][j]) for b in range(3) if b != a]
            row.append(csum(terms))
        v.append(row)
    out = []
    for i, j in OFF:
        t = csum([cmulc(v[a][j], w[a][i]) for a in range(3)])
        out += [t[0], t[1]]
    for i in range(2):
        s = None
        for a in range(3):
            p = v[a][i][1] * w[a][i][0] - v[a][i][0] * w[a][i][1]
            s = p if s is None else s + p
        out.append(s)
    return out


class Sites:
    def __init__(self):
        rows = lax.broadcasted_iota(jnp.int32, (4, 128), 0)
        lanes = lax.broadcasted_iota(jnp.int32, (4, 128), 1)
        self.first = (rows < 2, rows % 2 == 0, lanes < 64)
        self.y_last = lanes % 64 == 63
        self.y_first = lanes % 64 == 0

    def swap(self, v, d):
        if d == R:
            return pltpu.roll(v, 64, 1)
        if d == T:
            return jnp.concatenate([v[2:4], v[0:2]], axis=0)
        return jnp.where(
            self.first[Z],
            jnp.concatenate([v[1:4], v[0:1]], axis=0),
            jnp.concatenate([v[3:4], v[0:3]], axis=0),
        )

    def pack_low(self, a, b, d):
        return jnp.where(self.first[d], a, self.swap(b, d))

    def pack_high(self, a, b, d):
        return jnp.where(self.first[d], self.swap(b, d), a)

    def ahead(self, a, b, m, d):
        return (
            self.swap(jnp.where(self.first[d], m, a), d),
            jnp.where(self.first[d], self.swap(b, d), m),
        )

    def behind(self, a, b, m, d):
        return (
            self.swap(jnp.where(self.first[d], a, m), d),
            jnp.where(self.first[d], m, self.swap(b, d)),
        )

    def y_ahead(self, v):
        return jnp.where(self.y_last, pltpu.roll(v, 63, 1), pltpu.roll(v, 127, 1))

    def y_behind(self, v):
        return jnp.where(self.y_first, pltpu.roll(v, 65, 1), pltpu.roll(v, 1, 1))


def link(ref, mu, rows=3):
    return [[tuple(ref[(mu * 2 + c) * 9 + a * 3 + b] for c in range(2)) for b in range(3)] for a in range(rows)]


def spinor(ref, n, s, c):
    return tuple(ref[((n * 2 + k) * 4 + s) * 3 + c] for k in range(2))


def upper(ref, mu, sign, n, s, c):
    col, phase = BLOCKS[mu][s]
    return add_phase(spinor(ref, n, s, c), sign * phase, spinor(ref, n, 2 + col, c))


def half(ref, mu, sign):
    return {k: upper(ref, mu, sign, *k) for k in SPINS}


def flat_half(h):
    return [h[k][c] for k in SPINS for c in range(2)]


def unflat_half(flat):
    return {k: (flat[2 * i], flat[2 * i + 1]) for i, k in enumerate(SPINS)}


def apply(m, h):
    return {(n, s, a): csum([cmul(m[a][b], h[n, s, b]) for b in range(3)]) for n, s, a in SPINS}


def apply_dagger(m, h):
    return {(n, s, a): csum([cmulc(h[n, s, b], m[b][a]) for b in range(3)]) for n, s, a in SPINS}


def others(d):
    return [nu for nu in range(4) if nu != d]


def row_values(lref, nus):
    out = []
    for nu in nus:
        m = link(lref, nu, 2)
        out += [m[a][b][c] for a, b in ROWS for c in range(2)]
    return out


def rows_of(flat):
    return [[(flat[(a * 3 + b) * 2], flat[(a * 3 + b) * 2 + 1]) for b in range(3)] for a in range(2)]


def put(ref, at, flat):
    for i, v in enumerate(flat):
        ref[at + i] = v


def get(ref, at, n):
    return [ref[at + i] for i in range(n)]


LOW_LINKS, LOW = 18, 30
HIGH_LINKS, HIGH = 24, 36
AGAIN = 16


def pack_kernel(flags, lhbm, xhbm, zd, zu, ta, tb, rd, ru, gref, lref, xref, sems):
    copies = [
        pltpu.make_async_copy(xhbm, xref, sems.at[0]),
        pltpu.make_async_copy(lhbm, lref, sems.at[1]),
    ]
    for c in copies:
        c.start()
    sites = Sites()
    for c in copies:
        c.wait()
    for d in (Z, T, R):
        g = flat_half(apply_dagger(link(lref, d), half(xref, d, 1)))
        put(gref, 24 * d, g)
        low = row_values(lref, others(d)) + flat_half(half(xref, d, -1))
        high = row_values(lref, range(4)) + g
        low = [sites.pack_low(low[2 * i], low[2 * i + 1], d) for i in range(LOW)]
        high = [sites.pack_high(high[2 * i], high[2 * i + 1], d) for i in range(HIGH)]
        if d != T:
            put(zd if d == Z else rd, 0, low)
            put(zu if d == Z else ru, 0, high)
            continue
        low = low[:LOW_LINKS] + [jnp.where(flags[0] == 0, -v, v) for v in low[LOW_LINKS:]]
        high = high[:HIGH_LINKS] + [jnp.where(flags[1] == 0, -v, v) for v in high[HIGH_LINKS:]]
        even = flags[2] == 1
        for i in range(HIGH):
            x = low[i] if i < LOW else high[i]
            ta[i] = jnp.where(even, high[i], x)
            tb[i] = jnp.where(even, x, high[i])


class Halo:
    def __init__(self, flags, zd, zu, ta, tb, rd, ru):
        self.even = None if flags is None else flags[2] == 1
        self.refs = {Z: (zd, zu), T: (ta, tb), R: (rd, ru)}

    def low(self, d, i):
        first, second = self.refs[d]
        return jnp.where(self.even, first[i], second[i]) if d == T else first[i]

    def high(self, d, i):
        first, second = self.refs[d]
        return jnp.where(self.even, second[i], first[i]) if d == T else second[i]

    def ahead(self, sites, d, own, at):
        out = []
        for i in range(len(own) // 2):
            out += sites.ahead(own[2 * i], own[2 * i + 1], self.low(d, at + i), d)
        return out

    def behind(self, sites, d, own, at):
        out = []
        for i in range(len(own) // 2):
            out += sites.behind(own[2 * i], own[2 * i + 1], self.high(d, at + i), d)
        return out


def store_spinor(ref, n, s, c, value):
    for k in range(2):
        ref[((n * 2 + k) * 4 + s) * 3 + c] = value[k]


def mat_at(ref, at):
    return [[(ref[at + (a * 3 + b) * 2], ref[at + (a * 3 + b) * 2 + 1]) for b in range(3)] for a in range(3)]


def put_mat(ref, at, m):
    put(ref, at, [m[a][b][c] for a in range(3) for b in range(3) for c in range(2)])


def add_hops(yref, d, w, g):
    for n in range(2):
        for s in range(2):
            for c in range(3):
                y = spinor(yref, n, s, c)
                store_spinor(yref, n, s, c, [y[i] - HOPPING * (w[n, s, c][i] + g[n, s, c][i]) for i in range(2)])
        for r in range(2):
            col, phase = BLOCKS[d][r]
            for c in range(3):
                diff = [HOPPING * (g[n, r, c][i] - w[n, r, c][i]) for i in range(2)]
                y = add_phase(spinor(yref, n, 2 + col, c), -complex(phase).conjugate(), diff)
                store_spinor(yref, n, 2 + col, c, y)


def outer(p, q):
    return [
        [csum([cmulc(p[n, s, a], q[n, s, b]) for n in range(2) for s in range(2)]) for b in range(3)]
        for a in range(3)
    ]


def adjoint(m):
    return [[conj(m[b][a]) for b in range(3)] for a in range(3)]


def su3(left, right):
    return third_row([[csum([cmul(left[a][k], right[k][b]) for k in range(3)]) for b in range(3)] for a in range(2)])


def y_ahead(sites, m):
    return [[tuple(sites.y_ahead(v) for v in e) for e in row] for row in m]


def lower_y(sites, u_y, b_d, b_y):
    return antihermitian(matmul(u_y, su3(adjoint(y_ahead(sites, b_d)), su3(adjoint(b_y), b_d))), PLAQUETTE)


def scaled(m):
    return [[(PLAQUETTE * e[0], PLAQUETTE * e[1]) for e in row] for row in m]


def plane(sites, base, mu, nu, m1, m2, u_y):
    def add(at, part):
        base[at] = [a + b for a, b in zip(base[at], part)]

    p = antihermitian(matmul_dagger(m1, m2), PLAQUETTE)
    add(mu, p)
    add(nu, [-v for v in p])
    if nu == Y:
        add(mu, [-sites.y_behind(v) for v in transport(p, u_y)])


def early_kernel(lref, xref, gref, rd, ru, oy, ow, og, ob, om2, of, oq, obase):
    sites = Sites()
    halo = Halo(None, None, None, None, None, rd, ru)
    u = link(lref, Y)
    put(oy, 0, [xref[i] for i in range(48)])
    h = {k: tuple(sites.y_ahead(v) for v in c) for k, c in half(xref, Y, -1).items()}
    w = apply(u, h)
    g = {k: tuple(sites.y_behind(v) for v in c) for k, c in apply_dagger(u, half(xref, Y, 1)).items()}
    put(ow, 24, flat_half(w))
    put(og, 24, flat_half(g))
    add_hops(oy, Y, w, g)
    for mu in (T, Z):
        put_mat(om2, 18 * mu, su3(u, y_ahead(sites, link(lref, mu))))
    h = unflat_half(halo.ahead(sites, R, flat_half(half(xref, R, -1)), LOW_LINKS))
    g = unflat_half(halo.behind(sites, R, get(gref, 24 * R, 24), HIGH_LINKS))
    w = apply(link(lref, R), h)
    put(ow, 0, flat_half(w))
    put(og, 0, flat_half(g))
    add_hops(oy, R, w, g)
    flat = halo.ahead(sites, R, row_values(lref, others(R)), 0)
    f = [third_row(rows_of(flat[12 * k : 12 * k + 12])) for k in range(3)]
    put_mat(of, 0, f[0])
    put_mat(of, 18, f[1])
    base = [[0.0] * 8 for _ in range(4)]
    plane(sites, base, R, Y, su3(link(lref, R), f[2]), su3(u, y_ahead(sites, link(lref, R))), u)
    flat = halo.behind(sites, R, row_values(lref, range(4)), 0)
    put(ob, 0, flat[12 * R : 12 * R + 12])
    b = [third_row(rows_of(flat[12 * nu : 12 * nu + 12])) for nu in range(4)]
    for k in (T, Z):
        put_mat(oq, 18 * k, scaled(su3(adjoint(b[k]), b[R])))
    low = lower_y(sites, u, b[R], b[Y])
    put(obase, 0, base[R])
    put(obase, 8, [p + q for p, q in zip(base[Y], low)])


def depth_kernel(lref, xref, gref, yref, m2ref, fxref, bxyref, zd, zu, oy, ow, og, ob, of, oq, obase):
    sites = Sites()
    halo = Halo(None, zd, zu, None, None, None, None)
    u = link(lref, Y)
    put(oy, 0, get(yref, 0, 48))
    h = unflat_half(halo.ahead(sites, Z, flat_half(half(xref, Z, -1)), LOW_LINKS))
    g = unflat_half(halo.behind(sites, Z, get(gref, 24 * Z, 24), HIGH_LINKS))
    w = apply(link(lref, Z), h)
    put(ow, 0, flat_half(w))
    put(og, 0, flat_half(g))
    add_hops(oy, Z, w, g)
    flat = halo.ahead(sites, Z, row_values(lref, others(Z)), 0)
    f = [third_row(rows_of(flat[12 * k : 12 * k + 12])) for k in range(3)]
    put_mat(of, 0, f[0])
    base = [[0.0] * 8, [0.0] * 8, get(bxyref, 0, 8), get(bxyref, 8, 8)]
    plane(sites, base, Z, R, su3(link(lref, Z), f[1]), su3(link(lref, R), mat_at(fxref, 18)), u)
    plane(sites, base, Z, Y, su3(link(lref, Z), f[2]), mat_at(m2ref, 18), u)
    flat = halo.behind(sites, Z, row_values(lref, range(4)), 0)
    put(ob, 0, flat[12 * Z : 12 * Z + 12])
    b = [third_row(rows_of(flat[12 * nu : 12 * nu + 12])) for nu in range(4)]
    for k, mu in enumerate((T, R)):
        put_mat(oq, 18 * k, scaled(su3(adjoint(b[mu]), b[Z])))
    low = lower_y(sites, u, b[Z], b[Y])
    put(obase, 0, base[Z])
    put(obase, 8, base[R])
    put(obase, 16, [p + q for p, q in zip(base[Y], low)])


def partner_kernel(flags, lref, xref, gref, yinref, gxref, gzref, bxref, bzref, ta, tb, oz, ot, orow, oy, ow, on, ob):
    sites = Sites()
    halo = Halo(flags, None, None, ta, tb, None, None)
    put(oy, 0, get(yinref, 0, 48))
    h = unflat_half(halo.ahead(sites, T, flat_half(half(xref, T, -1)), LOW_LINKS))
    g = unflat_half(halo.behind(sites, T, get(gref, 24 * T, 24), HIGH_LINKS))
    w = apply(link(lref, T), h)
    put(ow, 0, flat_half(w))
    add_hops(oy, T, w, g)
    kept = {T: g, Z: unflat_half(get(gzref, 0, 24)), R: unflat_half(get(gxref, 0, 24))}
    rows = {T: halo.behind(sites, T, row_values(lref, (T,)), 6 * T), Z: get(bzref, 0, 12), R: get(bxref, 0, 12)}
    put(ob, 0, rows[T])
    for mu in (Z, T, R):
        part = antihermitian(outer(half(oy, mu, 1), kept[mu]), HOPPING)
        put(on, 8 * mu, part)
        moved = part + [v for d in range(3) if d != mu for v in rows[d]]
        ref = {Z: oz, T: ot, R: orow}[mu]
        put(ref, 0, [sites.pack_low(moved[2 * i], moved[2 * i + 1], mu) for i in range(AGAIN)])


def gauge_kernel(flags, lref, yref, wref, wzref, wxyref, gxyref, m2ref, fxref, fzref, bzxyref, ta, tb, obase, oq):
    sites = Sites()
    halo = Halo(flags, None, None, ta, tb, None, None)
    u = link(lref, Y)
    flat = halo.ahead(sites, T, row_values(lref, others(T)), 0)
    f = [third_row(rows_of(flat[12 * k : 12 * k + 12])) for k in range(3)]
    base = [[0.0] * 8] + [get(bzxyref, 8 * k, 8) for k in range(3)]

    def add(mu, part):
        base[mu] = [a + b for a, b in zip(base[mu], part)]

    for nu in (Z, R, Y):
        m1 = su3(link(lref, T), f[nu - 1])
        m2 = mat_at(m2ref, 0) if nu == Y else su3(link(lref, nu), mat_at(fzref if nu == Z else fxref, 0))
        plane(sites, base, T, nu, m1, m2, u)
    flat = halo.behind(sites, T, row_values(lref, range(4)), 0)
    b = [third_row(rows_of(flat[12 * nu : 12 * nu + 12])) for nu in range(4)]
    for k, mu in enumerate((Z, R)):
        put_mat(oq, 18 * k, scaled(su3(adjoint(b[mu]), b[T])))
    add(Y, lower_y(sites, u, b[T], b[Y]))
    for mu, (ref, at) in enumerate(((wref, 0), (wzref, 0), (wxyref, 0), (wxyref, 24))):
        add(mu, antihermitian(outer(unflat_half(get(ref, at, 24)), half(yref, mu, -1)), HOPPING))
    part = antihermitian(outer(half(yref, Y, 1), unflat_half(get(gxyref, 24, 24))), HOPPING)
    add(Y, transport([sites.y_ahead(v) for v in part], adjoint(u)))
    for mu in range(4):
        put(obase, 8 * mu, base[mu])


def times_dagger(x, u):
    e = {}
    for i, (a, b) in enumerate(OFF):
        e[a, b] = (x[2 * i], x[2 * i + 1])
        e[b, a] = (-x[2 * i], x[2 * i + 1])
    d = (x[6], x[7], -(x[6] + x[7]))
    return [
        [
            csum([(d[a] * u[j][a][1], d[a] * u[j][a][0])] + [cmulc(e[a, b], u[j][b]) for b in range(3) if b != a])
            for j in range(3)
        ]
        for a in range(3)
    ]


def last_kernel(lref, baseref, nref, btref, bzref, bxref, qtref, qzref, qxref, zd, td, rd, oref):
    sites = Sites()
    zero = jnp.zeros((4, 128), jnp.float32)
    for mu in range(4):
        x = get(baseref, 8 * mu, 8)
        if mu != Y:
            m = {Z: zd, T: td, R: rd}[mu]
            others_of = [d for d in range(3) if d != mu]
            own = get(nref, 8 * mu, 8) + [v for d in others_of for v in get((btref, bzref, bxref)[d], 0, 12)]
            ahead = []
            for i in range(AGAIN):
                ahead += sites.ahead(own[2 * i], own[2 * i + 1], m[i], mu)
            u = link(lref, mu)
            total = times_dagger(ahead[:8], u)
            for k, d in enumerate(others_of):
                c = third_row(rows_of(ahead[8 + 12 * k : 20 + 12 * k]))
                q = mat_at((qtref, qzref, qxref)[d], 18 * [e for e in range(3) if e != d].index(mu))
                v = matmul(adjoint(c), q)
                total = [[csum([total[a][b], v[a][b]]) for b in range(3)] for a in range(3)]
            x = [p + q for p, q in zip(x, antihermitian(matmul(u, total), 1.0))]
        at = mu * 18
        for i, (a, b) in enumerate(OFF):
            oref[at + a * 3 + b] = x[2 * i]
            oref[at + b * 3 + a] = -x[2 * i]
            oref[at + 9 + a * 3 + b] = x[2 * i + 1]
            oref[at + 9 + b * 3 + a] = x[2 * i + 1]
        for a in range(3):
            oref[at + a * 4] = zero
        oref[at + 9] = x[6]
        oref[at + 13] = x[7]
        oref[at + 17] = -(x[6] + x[7])


def call(body, operands, outs, flops, scratch=(), hbm=(), sems=0):
    specs = [
        pl.BlockSpec(
            memory_space=pltpu.SMEM if o.dtype == jnp.int32 else pltpu.HBM if i in hbm else pltpu.VMEM
        )
        for i, o in enumerate(operands)
    ]
    scratch = [pltpu.VMEM((n, 4, 128), jnp.float32) for n in scratch]
    return pl.pallas_call(
        body,
        in_specs=specs,
        out_specs=[pl.BlockSpec(memory_space=pltpu.VMEM) for _ in outs],
        out_shape=[jax.ShapeDtypeStruct((n, 4, 128), jnp.float32) for n in outs],
        scratch_shapes=scratch + ([pltpu.SemaphoreType.DMA((sems,))] if sems else []),
        cost_estimate=pl.CostEstimate(flops=flops, bytes_accessed=4 * 512 * 200, transcendentals=0),
        compiler_params=pltpu.CompilerParams(vmem_limit_bytes=8 * 1024 * 1024),
        interpret=INTERPRET,
    )(*operands)


def move(x, axis, by):
    size = lax.axis_size(axis)
    return lax.ppermute(x, axis, [(i, (i + by) % size) for i in range(size)])


def meet(x, axis, first):
    size = lax.axis_size(axis)
    pairs = []
    for i in range(0 if first else 1, size, 2):
        j = (i + 1) % size
        pairs += [(i, j), (j, i)]
    return lax.ppermute(x, axis, pairs)


def on_device(links, solutions):
    shape = links.shape
    lk = links.reshape(72, 4, 128)
    xs = solutions.reshape(48, 4, 128)
    t = lax.axis_index("ta")
    flags = jnp.stack([t, lax.axis_size("ta") - 1 - t, 1 - t % 2]).astype(jnp.int32)
    zd, zu, ta, tb, rd, ru, g, lk, xs = call(
        pack_kernel,
        (flags, pltpu.with_memory_space_constraint(lk, pltpu.HBM), pltpu.with_memory_space_constraint(xs, pltpu.HBM)),
        (LOW, HIGH, HIGH, HIGH, LOW, HIGH, 72, 72, 48),
        4_000_000,
        hbm=(1, 2),
        sems=2,
    )
    zu = move(zu, "gz", 1)
    zd = move(zd, "gz", -1)
    tb = meet(tb, "ta", False)
    ta = meet(ta, "ta", True)
    rd = move(rd, "xy", -1)
    ru = move(ru, "xy", 1)
    yl, wxy, gxy, bx, m2, fx, qx, bxy = call(
        early_kernel, (lk, xs, g, rd, ru), (48, 48, 48, 12, 36, 36, 36, 16), 20_000_000
    )
    yl, wz, gz, bz, fz, qz, bzxy = call(
        depth_kernel, (lk, xs, g, yl, m2, fx, bxy, zd, zu), (48, 24, 24, 12, 18, 36, 24), 20_000_000
    )
    oz, ot, orow, y, w, n, bt = call(
        partner_kernel,
        (flags, lk, xs, g, yl, gxy, gz, bx, bz, ta, tb),
        (AGAIN, AGAIN, AGAIN, 48, 24, 24, 12),
        20_000_000,
    )
    oz = move(oz, "gz", -1)
    ot = move(ot, "ta", -1)
    orow = move(orow, "xy", -1)
    base, qt = call(gauge_kernel, (flags, lk, y, w, wz, wxy, gxy, m2, fx, fz, bzxy, ta, tb), (32, 36), 20_000_000)
    (force,) = call(last_kernel, (lk, base, n, bt, bz, bx, qt, qz, qx, oz, ot, orow), (72,), 4_000_000)
    return force.reshape(shape)


def solution(mesh):
    spec = P(None, None, None, None, "ta", "gz", "xy")

    return jax.shard_map(on_device, mesh=mesh, in_specs=(spec, spec), out_specs=spec, check_vma=False)
```

```python
import jax
import jax.numpy as jnp
from jax import lax
from jax.experimental import pallas as pl
from jax.experimental.pallas import tpu as pltpu
from jax.sharding import PartitionSpec as P


HOPPING = 0.125
PLAQUETTE = 0.5
INTERPRET = False

BLOCKS = (
    ((0, 1), (1, 1)),
    ((0, 1j), (1, -1j)),
    ((1, 1j), (0, 1j)),
    ((1, -1), (0, 1)),
)
T, Z, R, Y = 0, 1, 2, 3
OFF = ((0, 1), (0, 2), (1, 2))
ROWS = tuple((a, b) for a in range(2) for b in range(3))
SPINS = tuple((n, s, c) for n in range(2) for s in range(2) for c in range(3))


def add_phase(a, phase, b):
    if phase == 1:
        return (a[0] + b[0], a[1] + b[1])
    if phase == -1:
        return (a[0] - b[0], a[1] - b[1])
    if phase == 1j:
        return (a[0] - b[1], a[1] + b[0])
    return (a[0] + b[1], a[1] - b[0])


def cmul(a, b):
    return (a[0] * b[0] - a[1] * b[1], a[0] * b[1] + a[1] * b[0])


def cmulc(a, b):
    return (a[0] * b[0] + a[1] * b[1], a[1] * b[0] - a[0] * b[1])


def conj(a):
    return (a[0], -a[1])


def csum(terms):
    re, im = terms[0]
    for t in terms[1:]:
        re, im = re + t[0], im + t[1]
    return (re, im)


def csub(a, b):
    return (a[0] - b[0], a[1] - b[1])


def matmul(left, right):
    return [[csum([cmul(left[a][k], right[k][b]) for k in range(3)]) for b in range(3)] for a in range(3)]


def matmul_dagger(left, right):
    return [[csum([cmulc(left[a][k], right[b][k]) for k in range(3)]) for b in range(3)] for a in range(3)]


def third_row(m):
    u, v = m
    cross = lambda i, j: conj(csub(cmul(u[i], v[j]), cmul(u[j], v[i])))
    return [u, v, [cross(1, 2), cross(2, 0), cross(0, 1)]]


def antihermitian(m, scale):
    out = []
    for a, b in OFF:
        out.append((0.5 * scale) * (m[a][b][0] - m[b][a][0]))
        out.append((0.5 * scale) * (m[a][b][1] + m[b][a][1]))
    third = (m[0][0][1] + m[1][1][1] + m[2][2][1]) * (1.0 / 3.0)
    out.append(scale * (m[0][0][1] - third))
    out.append(scale * (m[1][1][1] - third))
    return out


def transport(x, w):
    e = {}
    for i, (a, b) in enumerate(OFF):
        e[a, b] = (x[2 * i], x[2 * i + 1])
        e[b, a] = (-x[2 * i], x[2 * i + 1])
    d = (x[6], x[7], -(x[6] + x[7]))
    v = []
    for a in range(3):
        row = []
        for j in range(3):
            terms = [(-d[a] * w[a][j][1], d[a] * w[a][j][0])]
            terms += [cmul(e[a, b], w[b][j]) for b in range(3) if b != a]
            row.append(csum(terms))
        v.append(row)
    out = []
    for i, j in OFF:
        t = csum([cmulc(v[a][j], w[a][i]) for a in range(3)])
        out += [t[0], t[1]]
    for i in range(2):
        s = None
        for a in range(3):
            p = v[a][i][1] * w[a][i][0] - v[a][i][0] * w[a][i][1]
            s = p if s is None else s + p
        out.append(s)
    return out


class Sites:
    def __init__(self):
        rows = lax.broadcasted_iota(jnp.int32, (4, 128), 0)
        lanes = lax.broadcasted_iota(jnp.int32, (4, 128), 1)
        self.first = (rows < 2, rows % 2 == 0, lanes < 64)
        self.y_last = lanes % 64 == 63
        self.y_first = lanes % 64 == 0

    def swap(self, v, d):
        if d == R:
            return pltpu.roll(v, 64, 1)
        if d == T:
            return jnp.concatenate([v[2:4], v[0:2]], axis=0)
        return jnp.where(
            self.first[Z],
            jnp.concatenate([v[1:4], v[0:1]], axis=0),
            jnp.concatenate([v[3:4], v[0:3]], axis=0),
        )

    def pack_low(self, a, b, d):
        return jnp.where(self.first[d], a, self.swap(b, d))

    def pack_high(self, a, b, d):
        return jnp.where(self.first[d], self.swap(b, d), a)

    def ahead(self, a, b, m, d):
        return (
            self.swap(jnp.where(self.first[d], m, a), d),
            jnp.where(self.first[d], self.swap(b, d), m),
        )

    def behind(self, a, b, m, d):
        return (
            self.swap(jnp.where(self.first[d], a, m), d),
            jnp.where(self.first[d], m, self.swap(b, d)),
        )

    def y_ahead(self, v):
        return jnp.where(self.y_last, pltpu.roll(v, 63, 1), pltpu.roll(v, 127, 1))

    def y_behind(self, v):
        return jnp.where(self.y_first, pltpu.roll(v, 65, 1), pltpu.roll(v, 1, 1))


def link(ref, mu, rows=3):
    return [[tuple(ref[(mu * 2 + c) * 9 + a * 3 + b] for c in range(2)) for b in range(3)] for a in range(rows)]


def spinor(ref, n, s, c):
    return tuple(ref[((n * 2 + k) * 4 + s) * 3 + c] for k in range(2))


def upper(ref, mu, sign, n, s, c):
    col, phase = BLOCKS[mu][s]
    return add_phase(spinor(ref, n, s, c), sign * phase, spinor(ref, n, 2 + col, c))


def half(ref, mu, sign):
    return {k: upper(ref, mu, sign, *k) for k in SPINS}


def flat_half(h):
    return [h[k][c] for k in SPINS for c in range(2)]


def unflat_half(flat):
    return {k: (flat[2 * i], flat[2 * i + 1]) for i, k in enumerate(SPINS)}


def apply(m, h):
    return {(n, s, a): csum([cmul(m[a][b], h[n, s, b]) for b in range(3)]) for n, s, a in SPINS}


def apply_dagger(m, h):
    return {(n, s, a): csum([cmulc(h[n, s, b], m[b][a]) for b in range(3)]) for n, s, a in SPINS}


def others(d):
    return [nu for nu in range(4) if nu != d]


def row_values(lref, nus):
    out = []
    for nu in nus:
        m = link(lref, nu, 2)
        out += [m[a][b][c] for a, b in ROWS for c in range(2)]
    return out


def rows_of(flat):
    return [[(flat[(a * 3 + b) * 2], flat[(a * 3 + b) * 2 + 1]) for b in range(3)] for a in range(2)]


def put(ref, at, flat):
    for i, v in enumerate(flat):
        ref[at + i] = v


def get(ref, at, n):
    return [ref[at + i] for i in range(n)]


LOW_LINKS, LOW = 18, 30
LOW_LINKS_Z, LOW_Z = 12, 24
HIGH_LINKS, HIGH = 24, 36
AGAIN, AGAIN_Z = 16, 20


def pack_kernel(flags, lhbm, xhbm, zd, zu, ta, tb, rd, ru, gref, lref, xref, sems):
    copies = [
        pltpu.make_async_copy(xhbm, xref, sems.at[0]),
        pltpu.make_async_copy(lhbm, lref, sems.at[1]),
    ]
    for c in copies:
        c.start()
    sites = Sites()
    for c in copies:
        c.wait()
    for d in (Z, T, R):
        g = flat_half(apply_dagger(link(lref, d), half(xref, d, 1)))
        put(gref, 24 * d, g)
        low = row_values(lref, (T, R) if d == Z else others(d)) + flat_half(half(xref, d, -1))
        high = row_values(lref, range(4)) + g
        low = [sites.pack_low(low[2 * i], low[2 * i + 1], d) for i in range(len(low) // 2)]
        high = [sites.pack_high(high[2 * i], high[2 * i + 1], d) for i in range(HIGH)]
        if d != T:
            put(zd if d == Z else rd, 0, low)
            put(zu if d == Z else ru, 0, high)
            continue
        low = low[:LOW_LINKS] + [jnp.where(flags[0] == 0, -v, v) for v in low[LOW_LINKS:]]
        high = high[:HIGH_LINKS] + [jnp.where(flags[1] == 0, -v, v) for v in high[HIGH_LINKS:]]
        even = flags[2] == 1
        for i in range(HIGH):
            x = low[i] if i < LOW else high[i]
            ta[i] = jnp.where(even, high[i], x)
            tb[i] = jnp.where(even, x, high[i])


class Halo:
    def __init__(self, flags, zd, zu, ta, tb, rd, ru):
        self.even = None if flags is None else flags[2] == 1
        self.refs = {Z: (zd, zu), T: (ta, tb), R: (rd, ru)}

    def low(self, d, i):
        first, second = self.refs[d]
        return jnp.where(self.even, first[i], second[i]) if d == T else first[i]

    def high(self, d, i):
        first, second = self.refs[d]
        return jnp.where(self.even, second[i], first[i]) if d == T else second[i]

    def ahead(self, sites, d, own, at):
        out = []
        for i in range(len(own) // 2):
            out += sites.ahead(own[2 * i], own[2 * i + 1], self.low(d, at + i), d)
        return out

    def behind(self, sites, d, own, at):
        out = []
        for i in range(len(own) // 2):
            out += sites.behind(own[2 * i], own[2 * i + 1], self.high(d, at + i), d)
        return out


def store_spinor(ref, n, s, c, value):
    for k in range(2):
        ref[((n * 2 + k) * 4 + s) * 3 + c] = value[k]


def mat_at(ref, at):
    return [[(ref[at + (a * 3 + b) * 2], ref[at + (a * 3 + b) * 2 + 1]) for b in range(3)] for a in range(3)]


def put_mat(ref, at, m):
    put(ref, at, [m[a][b][c] for a in range(3) for b in range(3) for c in range(2)])


def add_hops(yref, d, w, g):
    for n in range(2):
        for s in range(2):
            for c in range(3):
                y = spinor(yref, n, s, c)
                store_spinor(yref, n, s, c, [y[i] - HOPPING * (w[n, s, c][i] + g[n, s, c][i]) for i in range(2)])
        for r in range(2):
            col, phase = BLOCKS[d][r]
            for c in range(3):
                diff = [HOPPING * (g[n, r, c][i] - w[n, r, c][i]) for i in range(2)]
                y = add_phase(spinor(yref, n, 2 + col, c), -complex(phase).conjugate(), diff)
                store_spinor(yref, n, 2 + col, c, y)


def outer(p, q):
    return [
        [csum([cmulc(p[n, s, a], q[n, s, b]) for n in range(2) for s in range(2)]) for b in range(3)]
        for a in range(3)
    ]


def adjoint(m):
    return [[conj(m[b][a]) for b in range(3)] for a in range(3)]


def su3(left, right):
    return third_row([[csum([cmul(left[a][k], right[k][b]) for k in range(3)]) for b in range(3)] for a in range(2)])


def y_ahead(sites, m):
    return [[tuple(sites.y_ahead(v) for v in e) for e in row] for row in m]


def lower_y(sites, u_y, b_d, b_y):
    return antihermitian(matmul(u_y, su3(adjoint(y_ahead(sites, b_d)), su3(adjoint(b_y), b_d))), PLAQUETTE)


def scaled(m):
    return [[(PLAQUETTE * e[0], PLAQUETTE * e[1]) for e in row] for row in m]


def plane(sites, base, mu, nu, m1, m2, u_y):
    def add(at, part):
        base[at] = [a + b for a, b in zip(base[at], part)]

    p = antihermitian(matmul_dagger(m1, m2), PLAQUETTE)
    add(mu, p)
    add(nu, [-v for v in p])
    if nu == Y:
        add(mu, [-sites.y_behind(v) for v in transport(p, u_y)])


def early_kernel(lref, xref, gref, rd, ru, oy, ow, og, ob, om2, of, oq, obase):
    sites = Sites()
    halo = Halo(None, None, None, None, None, rd, ru)
    u = link(lref, Y)
    put(oy, 0, [xref[i] for i in range(48)])
    h = {k: tuple(sites.y_ahead(v) for v in c) for k, c in half(xref, Y, -1).items()}
    w = apply(u, h)
    g = {k: tuple(sites.y_behind(v) for v in c) for k, c in apply_dagger(u, half(xref, Y, 1)).items()}
    put(ow, 24, flat_half(w))
    put(og, 24, flat_half(g))
    add_hops(oy, Y, w, g)
    put_mat(om2, 0, su3(u, y_ahead(sites, link(lref, T))))
    h = unflat_half(halo.ahead(sites, R, flat_half(half(xref, R, -1)), LOW_LINKS))
    g = unflat_half(halo.behind(sites, R, get(gref, 24 * R, 24), HIGH_LINKS))
    w = apply(link(lref, R), h)
    put(ow, 0, flat_half(w))
    put(og, 0, flat_half(g))
    add_hops(oy, R, w, g)
    flat = halo.ahead(sites, R, row_values(lref, others(R)), 0)
    f = [third_row(rows_of(flat[12 * k : 12 * k + 12])) for k in range(3)]
    put_mat(of, 0, f[0])
    put_mat(of, 18, f[1])
    base = [[0.0] * 8 for _ in range(4)]
    plane(sites, base, R, Y, su3(link(lref, R), f[2]), su3(u, y_ahead(sites, link(lref, R))), u)
    flat = halo.behind(sites, R, row_values(lref, range(4)), 0)
    put(ob, 0, flat[12 * R : 12 * R + 12])
    b = [third_row(rows_of(flat[12 * nu : 12 * nu + 12])) for nu in range(4)]
    for k in (T, Z):
        put_mat(oq, 18 * k, scaled(su3(adjoint(b[k]), b[R])))
    low = lower_y(sites, u, b[R], b[Y])
    put(obase, 0, base[R])
    put(obase, 8, [p + q for p, q in zip(base[Y], low)])


def depth_kernel(lref, xref, gref, yref, fxref, bxyref, zd, zu, oy, ow, og, ob, of, oq, obase, olow):
    sites = Sites()
    halo = Halo(None, zd, zu, None, None, None, None)
    u = link(lref, Y)
    put(oy, 0, get(yref, 0, 48))
    h = unflat_half(halo.ahead(sites, Z, flat_half(half(xref, Z, -1)), LOW_LINKS_Z))
    g = unflat_half(halo.behind(sites, Z, get(gref, 24 * Z, 24), HIGH_LINKS))
    w = apply(link(lref, Z), h)
    put(ow, 0, flat_half(w))
    put(og, 0, flat_half(g))
    add_hops(oy, Z, w, g)
    flat = halo.ahead(sites, Z, row_values(lref, (T, R)), 0)
    f = [third_row(rows_of(flat[12 * k : 12 * k + 12])) for k in range(2)]
    put_mat(of, 0, f[0])
    base = [[0.0] * 8, [0.0] * 8, get(bxyref, 0, 8), get(bxyref, 8, 8)]
    plane(sites, base, Z, R, su3(link(lref, Z), f[1]), su3(link(lref, R), mat_at(fxref, 18)), u)
    flat = halo.behind(sites, Z, row_values(lref, range(4)), 0)
    put(ob, 0, flat[12 * Z : 12 * Z + 12])
    b = [third_row(rows_of(flat[12 * nu : 12 * nu + 12])) for nu in range(4)]
    for k, mu in enumerate((T, R)):
        put_mat(oq, 18 * k, scaled(su3(adjoint(b[mu]), b[Z])))
    low = lower_y(sites, u, b[Z], b[Y])
    put(olow, 0, low)
    put(obase, 0, base[Z])
    put(obase, 8, base[R])
    put(obase, 16, [p + q for p, q in zip(base[Y], low)])


def partner_kernel(
    flags, lref, xref, gref, yinref, gxref, gzref, bxref, bzref, lowref, ta, tb, oz, ot, orow, oy, ow, on, ob
):
    sites = Sites()
    halo = Halo(flags, None, None, ta, tb, None, None)
    put(oy, 0, get(yinref, 0, 48))
    h = unflat_half(halo.ahead(sites, T, flat_half(half(xref, T, -1)), LOW_LINKS))
    g = unflat_half(halo.behind(sites, T, get(gref, 24 * T, 24), HIGH_LINKS))
    w = apply(link(lref, T), h)
    put(ow, 0, flat_half(w))
    add_hops(oy, T, w, g)
    kept = {T: g, Z: unflat_half(get(gzref, 0, 24)), R: unflat_half(get(gxref, 0, 24))}
    rows = {T: halo.behind(sites, T, row_values(lref, (T,)), 6 * T), Z: get(bzref, 0, 12), R: get(bxref, 0, 12)}
    put(ob, 0, rows[T])
    for mu in (Z, T, R):
        part = antihermitian(outer(half(oy, mu, 1), kept[mu]), HOPPING)
        put(on, 8 * mu, part)
        moved = part + [v for d in range(3) if d != mu for v in rows[d]]
        if mu == Z:
            moved += get(lowref, 0, 8)
        ref = {Z: oz, T: ot, R: orow}[mu]
        put(ref, 0, [sites.pack_low(moved[2 * i], moved[2 * i + 1], mu) for i in range(len(moved) // 2)])


def gauge_kernel(flags, lref, yref, wref, wzref, wxyref, gxyref, m2ref, fxref, fzref, bzxyref, ta, tb, obase, oq):
    sites = Sites()
    halo = Halo(flags, None, None, ta, tb, None, None)
    u = link(lref, Y)
    flat = halo.ahead(sites, T, row_values(lref, others(T)), 0)
    f = [third_row(rows_of(flat[12 * k : 12 * k + 12])) for k in range(3)]
    base = [[0.0] * 8] + [get(bzxyref, 8 * k, 8) for k in range(3)]

    def add(mu, part):
        base[mu] = [a + b for a, b in zip(base[mu], part)]

    for nu in (Z, R, Y):
        m1 = su3(link(lref, T), f[nu - 1])
        m2 = mat_at(m2ref, 0) if nu == Y else su3(link(lref, nu), mat_at(fzref if nu == Z else fxref, 0))
        plane(sites, base, T, nu, m1, m2, u)
    flat = halo.behind(sites, T, row_values(lref, range(4)), 0)
    b = [third_row(rows_of(flat[12 * nu : 12 * nu + 12])) for nu in range(4)]
    for k, mu in enumerate((Z, R)):
        put_mat(oq, 18 * k, scaled(su3(adjoint(b[mu]), b[T])))
    add(Y, lower_y(sites, u, b[T], b[Y]))
    for mu, (ref, at) in enumerate(((wref, 0), (wzref, 0), (wxyref, 0), (wxyref, 24))):
        add(mu, antihermitian(outer(unflat_half(get(ref, at, 24)), half(yref, mu, -1)), HOPPING))
    part = antihermitian(outer(half(yref, Y, 1), unflat_half(get(gxyref, 24, 24))), HOPPING)
    add(Y, transport([sites.y_ahead(v) for v in part], adjoint(u)))
    for mu in range(4):
        put(obase, 8 * mu, base[mu])


def times_dagger(x, u):
    e = {}
    for i, (a, b) in enumerate(OFF):
        e[a, b] = (x[2 * i], x[2 * i + 1])
        e[b, a] = (-x[2 * i], x[2 * i + 1])
    d = (x[6], x[7], -(x[6] + x[7]))
    return [
        [
            csum([(d[a] * u[j][a][1], d[a] * u[j][a][0])] + [cmulc(e[a, b], u[j][b]) for b in range(3) if b != a])
            for j in range(3)
        ]
        for a in range(3)
    ]


def last_kernel(lref, baseref, nref, btref, bzref, bxref, lowref, qtref, qzref, qxref, zd, td, rd, oref):
    sites = Sites()
    zero = jnp.zeros((4, 128), jnp.float32)
    base = [get(baseref, 8 * mu, 8) for mu in range(4)]
    for mu in range(4):
        x = base[mu]
        if mu != Y:
            m = {Z: zd, T: td, R: rd}[mu]
            others_of = [d for d in range(3) if d != mu]
            own = get(nref, 8 * mu, 8) + [v for d in others_of for v in get((btref, bzref, bxref)[d], 0, 12)]
            if mu == Z:
                own += get(lowref, 0, 8)
            ahead = []
            for i in range(len(own) // 2):
                ahead += sites.ahead(own[2 * i], own[2 * i + 1], m[i], mu)
            u = link(lref, mu)
            if mu == Z:
                p = transport(ahead[32:], adjoint(u))
                back = transport(p, link(lref, Y))
                x = [a + b - sites.y_behind(c) for a, b, c in zip(x, p, back)]
                base[Y] = [a - b for a, b in zip(base[Y], p)]
            total = times_dagger(ahead[:8], u)
            for k, d in enumerate(others_of):
                c = third_row(rows_of(ahead[8 + 12 * k : 20 + 12 * k]))
                q = mat_at((qtref, qzref, qxref)[d], 18 * [e for e in range(3) if e != d].index(mu))
                v = matmul(adjoint(c), q)
                total = [[csum([total[a][b], v[a][b]]) for b in range(3)] for a in range(3)]
            x = [p + q for p, q in zip(x, antihermitian(matmul(u, total), 1.0))]
        at = mu * 18
        for i, (a, b) in enumerate(OFF):
            oref[at + a * 3 + b] = x[2 * i]
            oref[at + b * 3 + a] = -x[2 * i]
            oref[at + 9 + a * 3 + b] = x[2 * i + 1]
            oref[at + 9 + b * 3 + a] = x[2 * i + 1]
        for a in range(3):
            oref[at + a * 4] = zero
        oref[at + 9] = x[6]
        oref[at + 13] = x[7]
        oref[at + 17] = -(x[6] + x[7])


def call(body, operands, outs, flops, scratch=(), hbm=(), sems=0):
    specs = [
        pl.BlockSpec(
            memory_space=pltpu.SMEM if o.dtype == jnp.int32 else pltpu.HBM if i in hbm else pltpu.VMEM
        )
        for i, o in enumerate(operands)
    ]
    scratch = [pltpu.VMEM((n, 4, 128), jnp.float32) for n in scratch]
    return pl.pallas_call(
        body,
        in_specs=specs,
        out_specs=[pl.BlockSpec(memory_space=pltpu.VMEM) for _ in outs],
        out_shape=[jax.ShapeDtypeStruct((n, 4, 128), jnp.float32) for n in outs],
        scratch_shapes=scratch + ([pltpu.SemaphoreType.DMA((sems,))] if sems else []),
        cost_estimate=pl.CostEstimate(flops=flops, bytes_accessed=4 * 512 * 200, transcendentals=0),
        compiler_params=pltpu.CompilerParams(vmem_limit_bytes=8 * 1024 * 1024),
        interpret=INTERPRET,
    )(*operands)


def move(x, axis, by):
    size = lax.axis_size(axis)
    return lax.ppermute(x, axis, [(i, (i + by) % size) for i in range(size)])


def meet(x, axis, first):
    size = lax.axis_size(axis)
    pairs = []
    for i in range(0 if first else 1, size, 2):
        j = (i + 1) % size
        pairs += [(i, j), (j, i)]
    return lax.ppermute(x, axis, pairs)


def on_device(links, solutions):
    shape = links.shape
    lk = links.reshape(72, 4, 128)
    xs = solutions.reshape(48, 4, 128)
    t = lax.axis_index("ta")
    flags = jnp.stack([t, lax.axis_size("ta") - 1 - t, 1 - t % 2]).astype(jnp.int32)
    zd, zu, ta, tb, rd, ru, g, lk, xs = call(
        pack_kernel,
        (flags, pltpu.with_memory_space_constraint(lk, pltpu.HBM), pltpu.with_memory_space_constraint(xs, pltpu.HBM)),
        (LOW_Z, HIGH, HIGH, HIGH, LOW, HIGH, 72, 72, 48),
        4_000_000,
        hbm=(1, 2),
        sems=2,
    )
    zu = move(zu, "gz", 1)
    zd = move(zd, "gz", -1)
    tb = meet(tb, "ta", False)
    ta = meet(ta, "ta", True)
    rd = move(rd, "xy", -1)
    ru = move(ru, "xy", 1)
    yl, wxy, gxy, bx, m2, fx, qx, bxy = call(
        early_kernel, (lk, xs, g, rd, ru), (48, 48, 48, 12, 18, 36, 36, 16), 20_000_000
    )
    yl, wz, gz, bz, fz, qz, bzxy, low = call(
        depth_kernel, (lk, xs, g, yl, fx, bxy, zd, zu), (48, 24, 24, 12, 18, 36, 24, 8), 20_000_000
    )
    oz, ot, orow, y, w, n, bt = call(
        partner_kernel,
        (flags, lk, xs, g, yl, gxy, gz, bx, bz, low, ta, tb),
        (AGAIN_Z, AGAIN, AGAIN, 48, 24, 24, 12),
        20_000_000,
    )
    oz = move(oz, "gz", -1)
    ot = move(ot, "ta", -1)
    orow = move(orow, "xy", -1)
    base, qt = call(gauge_kernel, (flags, lk, y, w, wz, wxy, gxy, m2, fx, fz, bzxy, ta, tb), (32, 36), 20_000_000)
    (force,) = call(last_kernel, (lk, base, n, bt, bz, bx, low, qt, qz, qx, oz, ot, orow), (72,), 4_000_000)
    return force.reshape(shape)


def solution(mesh):
    spec = P(None, None, None, None, "ta", "gz", "xy")

    return jax.shard_map(on_device, mesh=mesh, in_specs=(spec, spec), out_specs=spec, check_vma=False)
```

```python
import jax
import jax.numpy as jnp
from jax import lax
from jax.experimental import pallas as pl
from jax.experimental.pallas import tpu as pltpu
from jax.sharding import PartitionSpec as P


HOPPING = 0.125
PLAQUETTE = 0.5
INTERPRET = False

BLOCKS = (
    ((0, 1), (1, 1)),
    ((0, 1j), (1, -1j)),
    ((1, 1j), (0, 1j)),
    ((1, -1), (0, 1)),
)
T, Z, R, Y = 0, 1, 2, 3
OFF = ((0, 1), (0, 2), (1, 2))
ROWS = tuple((a, b) for a in range(2) for b in range(3))
SPINS = tuple((n, s, c) for n in range(2) for s in range(2) for c in range(3))


def add_phase(a, phase, b):
    if phase == 1:
        return (a[0] + b[0], a[1] + b[1])
    if phase == -1:
        return (a[0] - b[0], a[1] - b[1])
    if phase == 1j:
        return (a[0] - b[1], a[1] + b[0])
    return (a[0] + b[1], a[1] - b[0])


def cmul(a, b):
    return (a[0] * b[0] - a[1] * b[1], a[0] * b[1] + a[1] * b[0])


def cmulc(a, b):
    return (a[0] * b[0] + a[1] * b[1], a[1] * b[0] - a[0] * b[1])


def conj(a):
    return (a[0], -a[1])


def csum(terms):
    re, im = terms[0]
    for t in terms[1:]:
        re, im = re + t[0], im + t[1]
    return (re, im)


def csub(a, b):
    return (a[0] - b[0], a[1] - b[1])


def matmul(left, right):
    return [[csum([cmul(left[a][k], right[k][b]) for k in range(3)]) for b in range(3)] for a in range(3)]


def matmul_dagger(left, right):
    return [[csum([cmulc(left[a][k], right[b][k]) for k in range(3)]) for b in range(3)] for a in range(3)]


def third_row(m):
    u, v = m
    cross = lambda i, j: conj(csub(cmul(u[i], v[j]), cmul(u[j], v[i])))
    return [u, v, [cross(1, 2), cross(2, 0), cross(0, 1)]]


def antihermitian(m, scale):
    out = []
    for a, b in OFF:
        out.append((0.5 * scale) * (m[a][b][0] - m[b][a][0]))
        out.append((0.5 * scale) * (m[a][b][1] + m[b][a][1]))
    third = (m[0][0][1] + m[1][1][1] + m[2][2][1]) * (1.0 / 3.0)
    out.append(scale * (m[0][0][1] - third))
    out.append(scale * (m[1][1][1] - third))
    return out


def transport(x, w):
    e = {}
    for i, (a, b) in enumerate(OFF):
        e[a, b] = (x[2 * i], x[2 * i + 1])
        e[b, a] = (-x[2 * i], x[2 * i + 1])
    d = (x[6], x[7], -(x[6] + x[7]))
    v = []
    for a in range(3):
        row = []
        for j in range(3):
            terms = [(-d[a] * w[a][j][1], d[a] * w[a][j][0])]
            terms += [cmul(e[a, b], w[b][j]) for b in range(3) if b != a]
            row.append(csum(terms))
        v.append(row)
    out = []
    for i, j in OFF:
        t = csum([cmulc(v[a][j], w[a][i]) for a in range(3)])
        out += [t[0], t[1]]
    for i in range(2):
        s = None
        for a in range(3):
            p = v[a][i][1] * w[a][i][0] - v[a][i][0] * w[a][i][1]
            s = p if s is None else s + p
        out.append(s)
    return out


class Sites:
    def __init__(self):
        rows = lax.broadcasted_iota(jnp.int32, (4, 128), 0)
        lanes = lax.broadcasted_iota(jnp.int32, (4, 128), 1)
        self.first = (rows < 2, rows % 2 == 0, lanes < 64)
        self.y_last = lanes % 64 == 63
        self.y_first = lanes % 64 == 0

    def swap(self, v, d):
        if d == R:
            return pltpu.roll(v, 64, 1)
        if d == T:
            return jnp.concatenate([v[2:4], v[0:2]], axis=0)
        return jnp.where(
            self.first[Z],
            jnp.concatenate([v[1:4], v[0:1]], axis=0),
            jnp.concatenate([v[3:4], v[0:3]], axis=0),
        )

    def pack_low(self, a, b, d):
        return jnp.where(self.first[d], a, self.swap(b, d))

    def pack_high(self, a, b, d):
        return jnp.where(self.first[d], self.swap(b, d), a)

    def ahead(self, a, b, m, d):
        return (
            self.swap(jnp.where(self.first[d], m, a), d),
            jnp.where(self.first[d], self.swap(b, d), m),
        )

    def behind(self, a, b, m, d):
        return (
            self.swap(jnp.where(self.first[d], a, m), d),
            jnp.where(self.first[d], m, self.swap(b, d)),
        )

    def y_ahead(self, v):
        return jnp.where(self.y_last, pltpu.roll(v, 63, 1), pltpu.roll(v, 127, 1))

    def y_behind(self, v):
        return jnp.where(self.y_first, pltpu.roll(v, 65, 1), pltpu.roll(v, 1, 1))


def link(ref, mu, rows=3):
    return [[tuple(ref[(mu * 2 + c) * 9 + a * 3 + b] for c in range(2)) for b in range(3)] for a in range(rows)]


def spinor(ref, n, s, c):
    return tuple(ref[((n * 2 + k) * 4 + s) * 3 + c] for k in range(2))


def upper(ref, mu, sign, n, s, c):
    col, phase = BLOCKS[mu][s]
    return add_phase(spinor(ref, n, s, c), sign * phase, spinor(ref, n, 2 + col, c))


def half(ref, mu, sign):
    return {k: upper(ref, mu, sign, *k) for k in SPINS}


def flat_half(h):
    return [h[k][c] for k in SPINS for c in range(2)]


def unflat_half(flat):
    return {k: (flat[2 * i], flat[2 * i + 1]) for i, k in enumerate(SPINS)}


def apply(m, h):
    return {(n, s, a): csum([cmul(m[a][b], h[n, s, b]) for b in range(3)]) for n, s, a in SPINS}


def apply_dagger(m, h):
    return {(n, s, a): csum([cmulc(h[n, s, b], m[b][a]) for b in range(3)]) for n, s, a in SPINS}


def others(d):
    return [nu for nu in range(4) if nu != d]


def row_values(lref, nus):
    out = []
    for nu in nus:
        m = link(lref, nu, 2)
        out += [m[a][b][c] for a, b in ROWS for c in range(2)]
    return out


def rows_of(flat):
    return [[(flat[(a * 3 + b) * 2], flat[(a * 3 + b) * 2 + 1]) for b in range(3)] for a in range(2)]


def put(ref, at, flat):
    for i, v in enumerate(flat):
        ref[at + i] = v


def get(ref, at, n):
    return [ref[at + i] for i in range(n)]


LOW_LINKS, LOW = 18, 30
LOW_LINKS_Z, LOW_Z = 12, 24
HIGH_LINKS, HIGH = 24, 36
AGAIN, AGAIN_Z = 16, 20


def pack_kernel(flags, lhbm, xhbm, zd, zu, ta, tb, rd, ru, gref, lref, xref, sems):
    copies = [
        pltpu.make_async_copy(xhbm, xref, sems.at[0]),
        pltpu.make_async_copy(lhbm, lref, sems.at[1]),
    ]
    for c in copies:
        c.start()
    sites = Sites()
    for c in copies:
        c.wait()
    for d in (Z, T, R):
        g = flat_half(apply_dagger(link(lref, d), half(xref, d, 1)))
        put(gref, 24 * d, g)
        low = row_values(lref, (T, R) if d == Z else others(d)) + flat_half(half(xref, d, -1))
        high = row_values(lref, range(4)) + g
        low = [sites.pack_low(low[2 * i], low[2 * i + 1], d) for i in range(len(low) // 2)]
        high = [sites.pack_high(high[2 * i], high[2 * i + 1], d) for i in range(HIGH)]
        if d != T:
            put(zd if d == Z else rd, 0, low)
            put(zu if d == Z else ru, 0, high)
            continue
        low = low[:LOW_LINKS] + [jnp.where(flags[0] == 0, -v, v) for v in low[LOW_LINKS:]]
        high = high[:HIGH_LINKS] + [jnp.where(flags[1] == 0, -v, v) for v in high[HIGH_LINKS:]]
        even = flags[2] == 1
        for i in range(HIGH):
            x = low[i] if i < LOW else high[i]
            ta[i] = jnp.where(even, high[i], x)
            tb[i] = jnp.where(even, x, high[i])


class Halo:
    def __init__(self, flags, zd, zu, ta, tb, rd, ru):
        self.even = None if flags is None else flags[2] == 1
        self.refs = {Z: (zd, zu), T: (ta, tb), R: (rd, ru)}

    def low(self, d, i):
        first, second = self.refs[d]
        return jnp.where(self.even, first[i], second[i]) if d == T else first[i]

    def high(self, d, i):
        first, second = self.refs[d]
        return jnp.where(self.even, second[i], first[i]) if d == T else second[i]

    def ahead(self, sites, d, own, at):
        out = []
        for i in range(len(own) // 2):
            out += sites.ahead(own[2 * i], own[2 * i + 1], self.low(d, at + i), d)
        return out

    def behind(self, sites, d, own, at):
        out = []
        for i in range(len(own) // 2):
            out += sites.behind(own[2 * i], own[2 * i + 1], self.high(d, at + i), d)
        return out


def store_spinor(ref, n, s, c, value):
    for k in range(2):
        ref[((n * 2 + k) * 4 + s) * 3 + c] = value[k]


def mat_at(ref, at):
    return [[(ref[at + (a * 3 + b) * 2], ref[at + (a * 3 + b) * 2 + 1]) for b in range(3)] for a in range(3)]


def put_mat(ref, at, m):
    put(ref, at, [m[a][b][c] for a in range(3) for b in range(3) for c in range(2)])


def add_hops(yref, d, w, g):
    for n in range(2):
        for s in range(2):
            for c in range(3):
                y = spinor(yref, n, s, c)
                store_spinor(yref, n, s, c, [y[i] - HOPPING * (w[n, s, c][i] + g[n, s, c][i]) for i in range(2)])
        for r in range(2):
            col, phase = BLOCKS[d][r]
            for c in range(3):
                diff = [HOPPING * (g[n, r, c][i] - w[n, r, c][i]) for i in range(2)]
                y = add_phase(spinor(yref, n, 2 + col, c), -complex(phase).conjugate(), diff)
                store_spinor(yref, n, 2 + col, c, y)


def outer(p, q):
    return [
        [csum([cmulc(p[n, s, a], q[n, s, b]) for n in range(2) for s in range(2)]) for b in range(3)]
        for a in range(3)
    ]


def adjoint(m):
    return [[conj(m[b][a]) for b in range(3)] for a in range(3)]


def su3(left, right):
    return third_row([[csum([cmul(left[a][k], right[k][b]) for k in range(3)]) for b in range(3)] for a in range(2)])


def y_ahead(sites, m):
    return [[tuple(sites.y_ahead(v) for v in e) for e in row] for row in m]


def lower_y(sites, u_y, b_d, b_y):
    return antihermitian(matmul(u_y, su3(adjoint(y_ahead(sites, b_d)), su3(adjoint(b_y), b_d))), PLAQUETTE)


def scaled(m):
    return [[(PLAQUETTE * e[0], PLAQUETTE * e[1]) for e in row] for row in m]


def plane(sites, base, mu, nu, m1, m2, u_y):
    def add(at, part):
        base[at] = [a + b for a, b in zip(base[at], part)]

    p = antihermitian(matmul_dagger(m1, m2), PLAQUETTE)
    add(mu, p)
    add(nu, [-v for v in p])
    if nu == Y:
        add(mu, [-sites.y_behind(v) for v in transport(p, u_y)])


def early_kernel(lref, xref, gref, rd, ru, oy, ow, og, ob, om2, of, oq, obase):
    sites = Sites()
    halo = Halo(None, None, None, None, None, rd, ru)
    u = link(lref, Y)
    put(oy, 0, [xref[i] for i in range(48)])
    h = {k: tuple(sites.y_ahead(v) for v in c) for k, c in half(xref, Y, -1).items()}
    w = apply(u, h)
    g = {k: tuple(sites.y_behind(v) for v in c) for k, c in apply_dagger(u, half(xref, Y, 1)).items()}
    put(ow, 24, flat_half(w))
    put(og, 24, flat_half(g))
    add_hops(oy, Y, w, g)
    put_mat(om2, 0, su3(u, y_ahead(sites, link(lref, T))))
    h = unflat_half(halo.ahead(sites, R, flat_half(half(xref, R, -1)), LOW_LINKS))
    g = unflat_half(halo.behind(sites, R, get(gref, 24 * R, 24), HIGH_LINKS))
    w = apply(link(lref, R), h)
    put(ow, 0, flat_half(w))
    put(og, 0, flat_half(g))
    add_hops(oy, R, w, g)
    flat = halo.ahead(sites, R, row_values(lref, others(R)), 0)
    f = [third_row(rows_of(flat[12 * k : 12 * k + 12])) for k in range(3)]
    put_mat(of, 0, f[0])
    put_mat(of, 18, f[1])
    base = [[0.0] * 8 for _ in range(4)]
    plane(sites, base, R, Y, su3(link(lref, R), f[2]), su3(u, y_ahead(sites, link(lref, R))), u)
    flat = halo.behind(sites, R, row_values(lref, range(4)), 0)
    put(ob, 0, flat[12 * R : 12 * R + 12])
    b = [third_row(rows_of(flat[12 * nu : 12 * nu + 12])) for nu in range(4)]
    for k in (T, Z):
        put_mat(oq, 18 * k, scaled(su3(adjoint(b[k]), b[R])))
    low = lower_y(sites, u, b[R], b[Y])
    put(obase, 0, base[R])
    put(obase, 8, [p + q for p, q in zip(base[Y], low)])


def depth_kernel(lref, xref, gref, yref, fxref, bxyref, zd, zu, oy, ow, og, ob, of, oq, obase, olow):
    sites = Sites()
    halo = Halo(None, zd, zu, None, None, None, None)
    u = link(lref, Y)
    put(oy, 0, get(yref, 0, 48))
    h = unflat_half(halo.ahead(sites, Z, flat_half(half(xref, Z, -1)), LOW_LINKS_Z))
    g = unflat_half(halo.behind(sites, Z, get(gref, 24 * Z, 24), HIGH_LINKS))
    w = apply(link(lref, Z), h)
    put(ow, 0, flat_half(w))
    put(og, 0, flat_half(g))
    add_hops(oy, Z, w, g)
    flat = halo.ahead(sites, Z, row_values(lref, (T, R)), 0)
    f = [third_row(rows_of(flat[12 * k : 12 * k + 12])) for k in range(2)]
    put_mat(of, 0, f[0])
    base = [[0.0] * 8, [0.0] * 8, get(bxyref, 0, 8), get(bxyref, 8, 8)]
    plane(sites, base, Z, R, su3(link(lref, Z), f[1]), su3(link(lref, R), mat_at(fxref, 18)), u)
    flat = halo.behind(sites, Z, row_values(lref, range(4)), 0)
    put(ob, 0, flat[12 * Z : 12 * Z + 12])
    b = [third_row(rows_of(flat[12 * nu : 12 * nu + 12])) for nu in range(4)]
    for k, mu in enumerate((T, R)):
        put_mat(oq, 18 * k, scaled(su3(adjoint(b[mu]), b[Z])))
    low = lower_y(sites, u, b[Z], b[Y])
    put(olow, 0, low)
    put(obase, 0, base[Z])
    put(obase, 8, base[R])
    put(obase, 16, [p + q for p, q in zip(base[Y], low)])


def partner_kernel(
    flags, lref, xref, gref, yinref, gxref, gzref, bxref, bzref, lowref, ta, tb, oz, ot, orow, oy, ow, on, ob
):
    sites = Sites()
    halo = Halo(flags, None, None, ta, tb, None, None)
    put(oy, 0, get(yinref, 0, 48))
    h = unflat_half(halo.ahead(sites, T, flat_half(half(xref, T, -1)), LOW_LINKS))
    g = unflat_half(halo.behind(sites, T, get(gref, 24 * T, 24), HIGH_LINKS))
    w = apply(link(lref, T), h)
    put(ow, 0, flat_half(w))
    add_hops(oy, T, w, g)
    kept = {T: g, Z: unflat_half(get(gzref, 0, 24)), R: unflat_half(get(gxref, 0, 24))}
    rows = {T: halo.behind(sites, T, row_values(lref, (T,)), 6 * T), Z: get(bzref, 0, 12), R: get(bxref, 0, 12)}
    put(ob, 0, rows[T])
    for mu in (Z, T, R):
        part = antihermitian(outer(half(oy, mu, 1), kept[mu]), HOPPING)
        put(on, 8 * mu, part)
        moved = part + [v for d in range(3) if d != mu for v in rows[d]]
        if mu == Z:
            moved += get(lowref, 0, 8)
        ref = {Z: oz, T: ot, R: orow}[mu]
        put(ref, 0, [sites.pack_low(moved[2 * i], moved[2 * i + 1], mu) for i in range(len(moved) // 2)])


def gauge_kernel(flags, lref, yref, wref, wzref, wxyref, gxyref, m2ref, fxref, fzref, bzxyref, ta, tb, obase, oq):
    sites = Sites()
    halo = Halo(flags, None, None, ta, tb, None, None)
    u = link(lref, Y)
    flat = halo.ahead(sites, T, row_values(lref, others(T)), 0)
    f = [third_row(rows_of(flat[12 * k : 12 * k + 12])) for k in range(3)]
    base = [[0.0] * 8] + [get(bzxyref, 8 * k, 8) for k in range(3)]

    def add(mu, part):
        base[mu] = [a + b for a, b in zip(base[mu], part)]

    for nu in (Z, R, Y):
        m1 = su3(link(lref, T), f[nu - 1])
        m2 = mat_at(m2ref, 0) if nu == Y else su3(link(lref, nu), mat_at(fzref if nu == Z else fxref, 0))
        plane(sites, base, T, nu, m1, m2, u)
    flat = halo.behind(sites, T, row_values(lref, range(4)), 0)
    b = [third_row(rows_of(flat[12 * nu : 12 * nu + 12])) for nu in range(4)]
    for k, mu in enumerate((Z, R)):
        put_mat(oq, 18 * k, scaled(su3(adjoint(b[mu]), b[T])))
    add(Y, lower_y(sites, u, b[T], b[Y]))
    for mu, (ref, at) in enumerate(((wref, 0), (wzref, 0), (wxyref, 0), (wxyref, 24))):
        add(mu, antihermitian(outer(unflat_half(get(ref, at, 24)), half(yref, mu, -1)), HOPPING))
    part = antihermitian(outer(half(yref, Y, 1), unflat_half(get(gxyref, 24, 24))), HOPPING)
    add(Y, transport([sites.y_ahead(v) for v in part], adjoint(u)))
    for mu in range(4):
        put(obase, 8 * mu, base[mu])


def times_dagger(x, u):
    e = {}
    for i, (a, b) in enumerate(OFF):
        e[a, b] = (x[2 * i], x[2 * i + 1])
        e[b, a] = (-x[2 * i], x[2 * i + 1])
    d = (x[6], x[7], -(x[6] + x[7]))
    return [
        [
            csum([(d[a] * u[j][a][1], d[a] * u[j][a][0])] + [cmulc(e[a, b], u[j][b]) for b in range(3) if b != a])
            for j in range(3)
        ]
        for a in range(3)
    ]


def last_kernel(lref, baseref, nref, btref, bzref, bxref, lowref, qtref, qzref, qxref, zd, td, rd, out, oref, sems):
    sites = Sites()
    zero = jnp.zeros((4, 128), jnp.float32)
    base = [get(baseref, 8 * mu, 8) for mu in range(4)]
    copies = []
    for mu in (Z, Y, T, R):
        x = base[mu]
        if mu != Y:
            m = {Z: zd, T: td, R: rd}[mu]
            others_of = [d for d in range(3) if d != mu]
            own = get(nref, 8 * mu, 8) + [v for d in others_of for v in get((btref, bzref, bxref)[d], 0, 12)]
            if mu == Z:
                own += get(lowref, 0, 8)
            ahead = []
            for i in range(len(own) // 2):
                ahead += sites.ahead(own[2 * i], own[2 * i + 1], m[i], mu)
            u = link(lref, mu)
            if mu == Z:
                p = transport(ahead[32:], adjoint(u))
                back = transport(p, link(lref, Y))
                x = [a + b - sites.y_behind(c) for a, b, c in zip(x, p, back)]
                base[Y] = [a - b for a, b in zip(base[Y], p)]
            total = times_dagger(ahead[:8], u)
            for k, d in enumerate(others_of):
                c = third_row(rows_of(ahead[8 + 12 * k : 20 + 12 * k]))
                q = mat_at((qtref, qzref, qxref)[d], 18 * [e for e in range(3) if e != d].index(mu))
                v = matmul(adjoint(c), q)
                total = [[csum([total[a][b], v[a][b]]) for b in range(3)] for a in range(3)]
            x = [p + q for p, q in zip(x, antihermitian(matmul(u, total), 1.0))]
        at = mu * 18
        for i, (a, b) in enumerate(OFF):
            oref[at + a * 3 + b] = x[2 * i]
            oref[at + b * 3 + a] = -x[2 * i]
            oref[at + 9 + a * 3 + b] = x[2 * i + 1]
            oref[at + 9 + b * 3 + a] = x[2 * i + 1]
        for a in range(3):
            oref[at + a * 4] = zero
        oref[at + 9] = x[6]
        oref[at + 13] = x[7]
        oref[at + 17] = -(x[6] + x[7])
        copy = pltpu.make_async_copy(oref.at[pl.ds(at, 18)], out.at[pl.ds(at, 18)], sems.at[mu])
        copy.start()
        copies.append(copy)
    for copy in copies:
        copy.wait()


def call(body, operands, outs, flops, scratch=(), hbm=(), sems=0, out_space=pltpu.VMEM):
    specs = [
        pl.BlockSpec(
            memory_space=pltpu.SMEM if o.dtype == jnp.int32 else pltpu.HBM if i in hbm else pltpu.VMEM
        )
        for i, o in enumerate(operands)
    ]
    scratch = [pltpu.VMEM((n, 4, 128), jnp.float32) for n in scratch]
    return pl.pallas_call(
        body,
        in_specs=specs,
        out_specs=[pl.BlockSpec(memory_space=out_space) for _ in outs],
        out_shape=[jax.ShapeDtypeStruct((n, 4, 128), jnp.float32) for n in outs],
        scratch_shapes=scratch + ([pltpu.SemaphoreType.DMA((sems,))] if sems else []),
        cost_estimate=pl.CostEstimate(flops=flops, bytes_accessed=4 * 512 * 200, transcendentals=0),
        compiler_params=pltpu.CompilerParams(vmem_limit_bytes=8 * 1024 * 1024),
        interpret=INTERPRET,
    )(*operands)


def move(x, axis, by):
    size = lax.axis_size(axis)
    return lax.ppermute(x, axis, [(i, (i + by) % size) for i in range(size)])


def meet(x, axis, first):
    size = lax.axis_size(axis)
    pairs = []
    for i in range(0 if first else 1, size, 2):
        j = (i + 1) % size
        pairs += [(i, j), (j, i)]
    return lax.ppermute(x, axis, pairs)


def on_device(links, solutions):
    shape = links.shape
    lk = links.reshape(72, 4, 128)
    xs = solutions.reshape(48, 4, 128)
    t = lax.axis_index("ta")
    flags = jnp.stack([t, lax.axis_size("ta") - 1 - t, 1 - t % 2]).astype(jnp.int32)
    zd, zu, ta, tb, rd, ru, g, lk, xs = call(
        pack_kernel,
        (flags, pltpu.with_memory_space_constraint(lk, pltpu.HBM), pltpu.with_memory_space_constraint(xs, pltpu.HBM)),
        (LOW_Z, HIGH, HIGH, HIGH, LOW, HIGH, 72, 72, 48),
        4_000_000,
        hbm=(1, 2),
        sems=2,
    )
    zu = move(zu, "gz", 1)
    zd = move(zd, "gz", -1)
    tb = meet(tb, "ta", False)
    ta = meet(ta, "ta", True)
    rd = move(rd, "xy", -1)
    ru = move(ru, "xy", 1)
    yl, wxy, gxy, bx, m2, fx, qx, bxy = call(
        early_kernel, (lk, xs, g, rd, ru), (48, 48, 48, 12, 18, 36, 36, 16), 20_000_000
    )
    yl, wz, gz, bz, fz, qz, bzxy, low = call(
        depth_kernel, (lk, xs, g, yl, fx, bxy, zd, zu), (48, 24, 24, 12, 18, 36, 24, 8), 20_000_000
    )
    oz, ot, orow, y, w, n, bt = call(
        partner_kernel,
        (flags, lk, xs, g, yl, gxy, gz, bx, bz, low, ta, tb),
        (AGAIN_Z, AGAIN, AGAIN, 48, 24, 24, 12),
        20_000_000,
    )
    oz = move(oz, "gz", -1)
    ot = move(ot, "ta", -1)
    orow = move(orow, "xy", -1)
    base, qt = call(gauge_kernel, (flags, lk, y, w, wz, wxy, gxy, m2, fx, fz, bzxy, ta, tb), (32, 36), 20_000_000)
    (force,) = call(
        last_kernel,
        (lk, base, n, bt, bz, bx, low, qt, qz, qx, oz, ot, orow),
        (72,),
        4_000_000,
        (72,),
        sems=4,
        out_space=pltpu.HBM,
    )
    return force.reshape(shape)


def solution(mesh):
    spec = P(None, None, None, None, "ta", "gz", "xy")

    return jax.shard_map(on_device, mesh=mesh, in_specs=(spec, spec), out_specs=spec, check_vma=False)
```
